256 devices in a mesh: parts: 2 (over z), rows: 128 (over x, y, core).
Axes of the slice: x: 8, y: 8, z: 2, core: 2. Of those that a mesh axis runs over, the one named last changes fastest.
The devices are a block of a 8x8x16 slice.
Arguments:
- pair: bfloat16 [512, 256, 128], P(('parts', 'rows')), parts along dimension 0, may hold values from -16 to 16
- mask: int32 [512], P('parts'), parts along dimension 0, may hold values from 0 to 1, as said below
- w_tri_in: bfloat16 [128, 512], replicated, may hold values from -0.5 to 0.5
- w_tri_gate: bfloat16 [128, 128], replicated, may hold values from -0.5 to 0.5
- w_tri_out: bfloat16 [128, 128], replicated, may hold values from -0.5 to 0.5
- w_qkv: bfloat16 [128, 384], replicated, may hold values from -0.5 to 0.5
- w_att_bias: bfloat16 [128, 4], replicated, may hold values from -80 to 80
- w_att_gate: bfloat16 [128, 128], replicated, may hold values from -0.5 to 0.5
- w_att_out: bfloat16 [128, 128], replicated, may hold values from -0.5 to 0.5
Outputs:
- updated: bfloat16 [512, 256, 128], P(('parts', 'rows')), parts along dimension 0
The draws below stay inside these ranges and needn't reach their ends.
There are 2 independent parts, one for each index of `parts`. The reference program is written for one: setup_inputs(seed, part) draws one part's arguments, and reference() takes and returns one part's arrays. A program takes and returns all parts, laid end to end along the dimension named above; an argument that names none is the same for every part. Nothing has to cross between parts.
Inputs may be any that keep to these rules, and one draw needn't show every extreme that they name: `mask`: 0 on every residue from some L on, with 128 <= L <= 255; before L each residue may be 1 or 0 (unresolved); residue 0 is always 1.
All inputs are finite; a program needn't handle non-finite values.
Results may differ from the reference program's by a relative error of at most 0.012.
Values may be sent and summed in bfloat16 or wider, within the bound.
A program may use at most 64 MiB of HBM per device.

```python
import jax
import jax.numpy as jnp
from jax import lax

CZ = 128
CH = 128
HEADS = 4
HEAD_DIM = 32
ROWS_DEV = 2
RES = 256


def draw_pair(key, part):
    base = jax.random.normal(jax.random.fold_in(key, 11), (RES, RES, CZ), jnp.float32)
    return jnp.clip(base, -16.0, 16.0).astype(jnp.bfloat16)


def draw_mask(key, part):
    length = jax.random.randint(jax.random.fold_in(key, 21), (), RES // 2, RES)
    resolved = jax.random.randint(jax.random.fold_in(key, 22), (RES,), 0, 8) != 0
    positions = jnp.arange(RES)
    keep = (positions < length) & (resolved | (positions == 0))
    return keep.astype(jnp.int32)


def draw_w_att_bias(key, part):
    base = jax.random.normal(jax.random.fold_in(key, 31), (CZ, HEADS), jnp.float32) * CZ ** (-0.5)
    return jnp.clip(base, -80.0, 80.0).astype(jnp.bfloat16)


def bell_draw(rng, shape, scale, most, held_as=jnp.bfloat16):
    values = scale * jax.random.normal(rng, shape, jnp.float32)
    return jnp.clip(values, min=-most, max=most).astype(held_as)


def setup_inputs(seed: int = 0, part: int = 0) -> dict:
    splits = jax.random.split(jax.random.key(seed), 10)
    part_keys = jax.random.split(jax.random.fold_in(splits[9], part), 10)
    return {
        "pair": draw_pair(jax.random.fold_in(jax.random.fold_in(splits[9], part), 71), part),
        "mask": draw_mask(jax.random.fold_in(jax.random.fold_in(splits[9], part), 71), part),
        "w_tri_in": bell_draw(splits[2], (CZ, 4 * CH), CZ ** -0.5, 0.5),
        "w_tri_gate": bell_draw(splits[3], (CZ, CZ), CZ ** -0.5, 0.5),
        "w_tri_out": bell_draw(splits[4], (CH, CZ), CH ** -0.5, 0.5),
        "w_qkv": bell_draw(splits[5], (CZ, 3 * HEADS * HEAD_DIM), CZ ** -0.5, 0.5),
        "w_att_bias": draw_w_att_bias(jax.random.fold_in(splits[9], 71), part),
        "w_att_gate": bell_draw(splits[7], (CZ, HEADS * HEAD_DIM), CZ ** -0.5, 0.5),
        "w_att_out": bell_draw(splits[8], (HEADS * HEAD_DIM, CZ), (HEADS * HEAD_DIM) ** -0.5, 0.5),
    }


EPSILON = 1e-05
MASK_PENALTY = 1000000000.0

def normalize(values, along_axis):
    values = values.astype(jnp.float32)
    center = lax.optimization_barrier(jnp.mean(values, axis=along_axis, keepdims=True))
    shifted = values - center
    spread = lax.optimization_barrier(jnp.mean(shifted * shifted, axis=along_axis, keepdims=True))
    return shifted * lax.rsqrt(spread + EPSILON)

def rounded(values):
    return lax.optimization_barrier(values.astype(jnp.bfloat16))

def attend(queries, key_rows, values, score_bias, key_penalty, score_scale):
    column_count = queries.shape[1]
    heads_here = queries.shape[2]
    block_size = max(1, 4 // heads_here)

    def reorder(tensor):
        return tensor.reshape(tensor.shape[0], column_count // block_size, block_size, heads_here, -1).transpose(1, 0, 2, 3, 4)

    def one_block(inputs):
        query_part, key_part, value_part = inputs
        scores = jnp.einsum('kbhd,ibhd->bhki', key_part.astype(jnp.float32), query_part.astype(jnp.float32)) * score_scale
        scores = scores + score_bias[None] + key_penalty[None, None, :, None]
        row_peak = lax.optimization_barrier(jnp.max(scores, axis=2, keepdims=True))
        weights = jnp.exp(scores - row_peak)
        weights = rounded(weights / lax.optimization_barrier(jnp.sum(weights, axis=2, keepdims=True)))
        result = jnp.einsum('bhki,kbhd->ibhd', weights.astype(jnp.float32), value_part.astype(jnp.float32))
        return result.astype(jnp.bfloat16)
    outputs = lax.map(one_block, (reorder(queries), reorder(key_rows), reorder(values)))
    return outputs.transpose(1, 0, 2, 3, 4).reshape(queries.shape)

def reference(pair, mask, w_tri_in, w_tri_gate, w_tri_out, w_qkv, w_att_bias, w_att_gate, w_att_out):
    key_mask = mask.astype(jnp.float32)
    key_penalty = (key_mask - 1.0) * MASK_PENALTY
    blocks = RES // ROWS_DEV
    row_masks = key_mask.reshape(blocks, ROWS_DEV)
    pair_blocks = pair.reshape(blocks, ROWS_DEV, RES, CZ)

    def first_section(inputs):
        pair_block, row_mask = inputs
        normed = rounded(normalize(pair_block, 2))
        projected = jnp.einsum('rkc,cf->frk', normed.astype(jnp.float32), w_tri_in.astype(jnp.float32))
        pair_mask = row_mask[:, None] * key_mask[None, :]
        left_side = (jax.nn.sigmoid(projected[:CH]) * projected[CH:2 * CH] * pair_mask).astype(jnp.bfloat16)
        right_side = (jax.nn.sigmoid(projected[2 * CH:3 * CH]) * projected[3 * CH:] * pair_mask).astype(jnp.bfloat16)
        return (left_side, right_side)
    left_blocks, right_blocks = lax.map(first_section, (pair_blocks, row_masks))
    left_full = left_blocks.transpose(1, 0, 2, 3).reshape(CH, RES, RES)
    right_full = right_blocks.transpose(1, 0, 2, 3).reshape(CH, RES, RES)

    def contract(inputs):
        left_piece, right_piece = inputs
        return jnp.dot(left_piece, right_piece.T, preferred_element_type=jnp.float32).astype(jnp.bfloat16)
    product = lax.map(contract, (left_full, right_full))
    product_blocks = product.reshape(CH, blocks, ROWS_DEV, RES).transpose(1, 0, 2, 3)

    def second_section(inputs):
        pair_block, triangle_rows = inputs
        normed = rounded(normalize(pair_block, 2))
        triangle_normed = rounded(normalize(triangle_rows, 0))
        triangle_gate = jax.nn.sigmoid(jnp.einsum('rjc,cd->rjd', normed.astype(jnp.float32), w_tri_gate.astype(jnp.float32)))
        triangle_update = jnp.einsum('crj,cd->rjd', triangle_normed.astype(jnp.float32), w_tri_out.astype(jnp.float32))
        middle = rounded(pair_block.astype(jnp.float32) + triangle_gate * triangle_update)
        attention_input = rounded(normalize(middle, 2))
        bias_rows = jnp.einsum('kic,ch->hki', attention_input.astype(jnp.float32), w_att_bias.astype(jnp.float32))
        projections = jnp.einsum('ijc,cf->ijf', attention_input.astype(jnp.float32), w_qkv.astype(jnp.float32)).astype(jnp.bfloat16)
        return (middle, bias_rows, projections)
    middle_blocks, biases, projection_blocks = lax.map(second_section, (pair_blocks, product_blocks))
    bias_full = biases.transpose(1, 0, 2, 3).reshape(HEADS, RES, RES)
    projections = projection_blocks.reshape(RES, RES, 3, HEADS, HEAD_DIM)
    attended = attend(projections[:, :, 0], projections[:, :, 1], projections[:, :, 2], bias_full, key_penalty, HEAD_DIM ** (-0.5))
    attended_blocks = attended.reshape(blocks, ROWS_DEV, RES, HEADS * HEAD_DIM)

    def third_section(inputs):
        middle, attention_rows = inputs
        attention_input = rounded(normalize(middle, 2))
        attention_gate = jax.nn.sigmoid(jnp.einsum('rjc,cf->rjf', attention_input.astype(jnp.float32), w_att_gate.astype(jnp.float32)))
        gated_output = rounded(attention_gate * attention_rows.astype(jnp.float32))
        result = middle.astype(jnp.float32) + jnp.einsum('rjf,fc->rjc', gated_output.astype(jnp.float32), w_att_out.astype(jnp.float32))
        return result.astype(jnp.bfloat16)
    outputs = lax.map(third_section, (middle_blocks, attended_blocks))
    return outputs.reshape(RES, RES, CZ)
```

```python
import functools

import jax
import jax.numpy as jnp
from jax import lax
from jax.experimental import pallas as pl
from jax.experimental.pallas import tpu as pltpu
from jax.sharding import PartitionSpec as P

HEADS = 4
HEAD_DIM = 32
EPSILON = 1e-05
MASK_PENALTY = 1000000000.0
MESH = pl.DeviceIdType.MESH
BF = jnp.bfloat16
F32 = jnp.float32
NN = (((1,), (0,)), ((), ()))
NT = (((1,), (1,)), ((), ()))
TN = (((0,), (0,)), ((), ()))


def dot(a, b, dims=NN):
    return lax.dot_general(a, b, dims, preferred_element_type=F32)


def sigmoid(x):
    return 0.5 * jnp.tanh(0.5 * x) + 0.5


def norm_lanes(x):
    center = jnp.mean(x, axis=1, keepdims=True)
    shifted = x - center
    spread = jnp.mean(shifted * shifted, axis=1, keepdims=True)
    return shifted * lax.rsqrt(spread + EPSILON)


def iota(shape, dim):
    return lax.broadcasted_iota(jnp.int32, shape, dim)


def spread_rows(rows, picked, parity):
    return (iota((rows, picked), 0) == 2 * iota((rows, picked), 1) + parity).astype(F32).astype(BF)


def whole_wait(ref, sem):
    pltpu.make_async_copy(ref, ref, sem).wait()


def kernel(
    n,
    pair_ref, mask_ref, w_in_ref, w_tg_ref, w_to_ref, w_qkv_ref, w_ab_ref, w_ag_ref, w_ao_ref,
    out_ref,
    pair_send, edge_send, edge_recv, pair_recv, prod_send, prod_recv, tokens, middle, att_own, att_peer,
    bias_send, bias_recv, scores, o_send, o_recv, o_own, upd_send, upd_recv,
    send_sem, recv_sem,
):
    rows, res, cz = pair_ref.shape
    me = lax.axis_index("rows")
    core = lax.rem(me, 2)
    partner = me + 1 - 2 * core

    barrier = pltpu.get_barrier_semaphore()

    def peer(t):
        return lax.rem(me + t, n)

    def greet(t, carry):
        pl.semaphore_signal(barrier, inc=1, device_id={"rows": peer(t)}, device_id_type=MESH)
        return carry

    lax.fori_loop(1, n, greet, 0)

    def exchange(source, target, k):
        def send(t, carry):
            d = peer(t)
            pltpu.make_async_remote_copy(
                src_ref=source(d), dst_ref=target, send_sem=send_sem.at[k], recv_sem=recv_sem.at[k],
                device_id={"rows": d}, device_id_type=MESH,
            ).start()
            return carry

        lax.fori_loop(1, n, send, 0)
        pltpu.make_async_copy(source(me), target, recv_sem.at[k]).start()

    def to_partner(source, target, k):
        copy = pltpu.make_async_remote_copy(
            src_ref=source, dst_ref=target, send_sem=send_sem.at[k], recv_sem=recv_sem.at[k],
            device_id={"rows": partner}, device_id_type=MESH,
        )
        copy.start()
        return copy

    key_mask = mask_ref[...].astype(F32)
    lane = iota((1, res), 1)
    row_mask = [
        jnp.sum(jnp.where(lane == me * rows + r, key_mask, 0.0), axis=1, keepdims=True) for r in range(rows)
    ]
    spreads = [spread_rows(2 * cz, cz, r) for r in range(2)]
    pair_send[...] = pair_ref[...].reshape(rows, n, 2, cz)
    normed = jnp.concatenate(
        [norm_lanes(pair_ref[r].astype(F32)).astype(BF) for r in range(rows)], axis=1
    )

    def projected(g):
        w = w_in_ref[:, g * cz : (g + 1) * cz]
        spread_w = jnp.concatenate([dot(s, w, NT).astype(BF) for s in spreads], axis=1)
        return dot(spread_w, normed, NT)

    parity = iota((2 * cz, res), 0) % 2
    pair_mask = jnp.where(parity == 0, row_mask[0], row_mask[1]) * key_mask
    for a in range(2):
        edge = (sigmoid(projected(2 * a)) * projected(2 * a + 1) * pair_mask).astype(BF)
        edge_send[:, a] = edge.reshape(n, 2, res)

    pl.semaphore_wait(barrier, n - 1)
    exchange(lambda d: edge_send.at[d], edge_recv.at[me], 0)
    exchange(lambda d: pair_send.at[:, d], pair_recv.at[me], 1)

    whole_wait(edge_recv, recv_sem.at[0])
    left = edge_recv[:, 0].reshape(res, res)
    right = edge_recv[:, 1].reshape(res, res)
    prod_send[...] = dot(right, left, NT).astype(BF).reshape(n, 2, res)
    exchange(lambda d: prod_send.at[d], prod_recv.at[me], 2)

    whole_wait(pair_recv, recv_sem.at[1])
    tokens[...] = pair_recv[...].reshape(2 * res, cz).astype(F32)
    columns = [tokens[pl.ds(jj, res, stride=2), :] for jj in range(2)]
    gates = [sigmoid(dot(norm_lanes(x).astype(BF), w_tg_ref[...])) for x in columns]
    w_to = w_to_ref[...]
    spread_out = jnp.concatenate([dot(s, w_to).astype(BF) for s in spreads], axis=1)
    e_row = iota((8, HEADS), 0)
    e_col = iota((8, HEADS), 1)
    w_bias = jnp.concatenate(
        [
            dot(((e_row // 2 == e_col) & (e_row % 2 == jj)).astype(F32).astype(BF), w_ab_ref[...], NT).astype(BF)
            for jj in range(2)
        ],
        axis=1,
    )

    whole_wait(prod_recv, recv_sem.at[2])
    product = prod_recv[...].reshape(2 * cz, res).astype(F32)
    sub = iota((8, res), 0) % 2

    def column_mean(x):
        total = jnp.sum(x.reshape(2 * cz // 8, 8, res), axis=0)
        even = jnp.sum(jnp.where(sub == 0, total, 0.0), axis=0, keepdims=True)
        odd = jnp.sum(jnp.where(sub == 0, 0.0, total), axis=0, keepdims=True)
        return jnp.where(sub == 0, even, odd) * (1.0 / cz)

    tall = product.reshape(2 * cz // 8, 8, res)
    tall = tall - column_mean(product)[None]
    spread = column_mean((tall * tall).reshape(2 * cz, res))
    tri = (tall * lax.rsqrt(spread + EPSILON)[None]).reshape(2 * cz, res).astype(BF)
    update = dot(tri, spread_out, TN)
    for jj in range(2):
        mid = (columns[jj] + gates[jj] * update[:, jj * cz : (jj + 1) * cz]).astype(BF).astype(F32)
        middle[jj] = mid
        att_own[jj] = norm_lanes(mid).astype(BF)
    to_partner(att_own, att_peer, 4)
    both = jnp.concatenate([att_own[0], att_own[1]], axis=1)
    bias_send[...] = dot(w_bias, both, NT).reshape(2, 4, res)
    exchange(lambda d: bias_send.at[lax.rem(d, 2)], bias_recv.at[me], 3)

    penalty = (key_mask - 1.0) * MASK_PENALTY
    lane_head = iota((1, cz), 1) // HEAD_DIM
    head_mask = [lane_head == 2 * core + h for h in range(2)]
    values = []
    for l in range(4):
        if l == 2:
            whole_wait(att_peer, recv_sem.at[4])
        x = att_own[l] if l < 2 else att_peer[l - 2]
        qkv = dot(x, w_qkv_ref[...]).astype(BF)
        for h in range(2):
            key = jnp.where(head_mask[h], qkv[:, cz : 2 * cz], 0)
            scores[2 * l + h] = dot(qkv[:, :cz], key, NT) * (HEAD_DIM ** -0.5) + penalty
        values.append(qkv[:, 2 * cz :])
    att_gates = [sigmoid(dot(att_own[jj], w_ag_ref[...])) for jj in range(2)]

    whole_wait(bias_recv, recv_sem.at[3])
    any_head = head_mask[0] | head_mask[1]

    def attended(l):
        total = None
        for h in range(2):
            s = scores[2 * l + h] + bias_recv[:, 2 * h : 2 * h + 2].reshape(res, res)
            e = jnp.exp(s - jnp.max(s, axis=1, keepdims=True)).astype(BF)
            ones = jnp.broadcast_to(jnp.where(head_mask[h], 1.0, 0.0), (res, cz)).astype(BF)
            part = dot(e, jnp.concatenate([jnp.where(head_mask[h], values[l], 0), ones], axis=1))
            total = part if total is None else total + part
        return (total[:, :cz] / jnp.where(any_head, total[:, cz:], 1.0)).astype(BF)

    for l in (2, 3):
        o_send[l - 2] = attended(l)
        to_partner(o_send.at[l - 2], o_recv.at[l - 2], 3 + l)
    for jj in range(2):
        o_own[jj] = attended(jj)
    for jj in range(2):
        whole_wait(o_recv.at[jj], recv_sem.at[5 + jj])
        att = o_own[jj].astype(F32) + o_recv[jj].astype(F32)
        gated = (att_gates[jj] * att).astype(BF)
        tokens[pl.ds(jj, res, stride=2), :] = middle[jj] + dot(gated, w_ao_ref[...])
    upd_send[...] = tokens[...].astype(BF).reshape(n, rows, 2, cz)
    exchange(lambda d: upd_send.at[d], upd_recv.at[:, me], 7)
    whole_wait(upd_recv, recv_sem.at[7])
    out_ref[...] = upd_recv[...].reshape(rows, res, cz)

    others = pl.ds(0, n - 1)
    whole_wait(edge_recv.at[others], send_sem.at[0])
    whole_wait(pair_recv.at[others], send_sem.at[1])
    whole_wait(prod_recv.at[others], send_sem.at[2])
    whole_wait(bias_recv.at[others], send_sem.at[3])
    whole_wait(att_peer, send_sem.at[4])
    whole_wait(o_recv.at[0], send_sem.at[5])
    whole_wait(o_recv.at[1], send_sem.at[6])
    whole_wait(upd_recv.at[:, others], send_sem.at[7])


def local(n, pair, mask, w_tri_in, w_tri_gate, w_tri_out, w_qkv, w_att_bias, w_att_gate, w_att_out):
    rows, res, cz = pair.shape
    vmem = pl.BlockSpec(memory_space=pltpu.VMEM)
    return pl.pallas_call(
        functools.partial(kernel, n),
        out_shape=jax.ShapeDtypeStruct(pair.shape, BF),
        in_specs=[vmem] * 9,
        out_specs=vmem,
        scratch_shapes=[
            pltpu.VMEM((rows, n, 2, cz), BF),
            pltpu.VMEM((n, 2, 2, res), BF),
            pltpu.VMEM((n, 2, 2, res), BF),
            pltpu.VMEM((n, rows, 2, cz), BF),
            pltpu.VMEM((n, 2, res), BF),
            pltpu.VMEM((n, 2, res), BF),
            pltpu.VMEM((2 * res, cz), F32),
            pltpu.VMEM((2, res, cz), F32),
            pltpu.VMEM((2, res, cz), BF),
            pltpu.VMEM((2, res, cz), BF),
            pltpu.VMEM((2, 4, res), F32),
            pltpu.VMEM((n, 4, res), F32),
            pltpu.VMEM((8, res, res), F32),
            pltpu.VMEM((2, res, cz), BF),
            pltpu.VMEM((2, res, cz), BF),
            pltpu.VMEM((2, res, cz), BF),
            pltpu.VMEM((n, rows, 2, cz), BF),
            pltpu.VMEM((rows, n, 2, cz), BF),
            pltpu.SemaphoreType.DMA((8,)),
            pltpu.SemaphoreType.DMA((8,)),
        ],
        compiler_params=pltpu.CompilerParams(collective_id=0, has_side_effects=True),
        name="pair_update",
    )(pair, mask.reshape(1, res), w_tri_in, w_tri_gate, w_tri_out, w_qkv, w_att_bias, w_att_gate, w_att_out)


def solution(mesh):
    split = P(("parts", "rows"), None, None)
    placed = (split, P("parts"), P(), P(), P(), P(), P(), P(), P())
    return jax.shard_map(
        functools.partial(local, mesh.shape["rows"]), mesh=mesh, in_specs=placed, out_specs=split, check_vma=False
    )
```

```python
import functools

import jax
import jax.numpy as jnp
from jax import lax
from jax.experimental import pallas as pl
from jax.experimental.pallas import tpu as pltpu
from jax.sharding import PartitionSpec as P

HEADS = 4
HEAD_DIM = 32
EPSILON = 1e-05
MASK_PENALTY = 1000000000.0
MESH = pl.DeviceIdType.MESH
BF = jnp.bfloat16
F32 = jnp.float32
NN = (((1,), (0,)), ((), ()))
NT = (((1,), (1,)), ((), ()))
TN = (((0,), (0,)), ((), ()))

import random


def far_first():
    order = [(x, y, c) for x in range(8) for y in range(8) for c in range(2) if x + y + c]
    random.Random(1).shuffle(order)
    return sorted(order, key=lambda o: -(min(o[0], 8 - o[0]) + min(o[1], 8 - o[1])))


ORDER = far_first()


def dot(a, b, dims=NN):
    return lax.dot_general(a, b, dims, preferred_element_type=F32)


def sigmoid(x):
    return 0.5 * jnp.tanh(0.5 * x) + 0.5


def norm_lanes(x):
    center = jnp.mean(x, axis=1, keepdims=True)
    shifted = x - center
    spread = jnp.mean(shifted * shifted, axis=1, keepdims=True)
    return shifted * lax.rsqrt(spread + EPSILON)


def iota(shape, dim):
    return lax.broadcasted_iota(jnp.int32, shape, dim)


def spread_rows(rows, picked, parity):
    return (iota((rows, picked), 0) == 2 * iota((rows, picked), 1) + parity).astype(F32).astype(BF)


def whole_wait(ref, sem):
    pltpu.make_async_copy(ref, ref, sem).wait()


def kernel(
    n,
    pair_ref, mask_ref, w_in_ref, w_tg_ref, w_to_ref, w_qkv_ref, w_ab_ref, w_ag_ref, w_ao_ref,
    out_ref,
    pair_send, edge_send, edge_recv, pair_recv, prod_send, prod_recv, tokens, middle, att_own, att_peer,
    bias_send, bias_recv, scores, o_send, o_recv, o_own, upd_send, upd_recv,
    send_sem, recv_sem,
):
    rows, res, cz = pair_ref.shape
    me = lax.axis_index("rows")
    core = lax.rem(me, 2)
    partner = me + 1 - 2 * core

    barrier = pltpu.get_barrier_semaphore()

    def peer(t):
        return lax.rem(me + t, n)

    def greet(t, carry):
        pl.semaphore_signal(barrier, inc=1, device_id={"rows": peer(t)}, device_id_type=MESH)
        return carry

    lax.fori_loop(1, n, greet, 0)

    def exchange(source, target, k):
        for tx, ty, tc in ORDER:
            d = (((me // 16 + tx) % 8) * 8 + (me // 2 + ty) % 8) * 2 + (core + tc) % 2
            pltpu.make_async_remote_copy(
                src_ref=source(d), dst_ref=target, send_sem=send_sem.at[k], recv_sem=recv_sem.at[k],
                device_id={"rows": d}, device_id_type=MESH,
            ).start()
        pltpu.make_async_copy(source(me), target, recv_sem.at[k]).start()

    def to_partner(source, target, k):
        copy = pltpu.make_async_remote_copy(
            src_ref=source, dst_ref=target, send_sem=send_sem.at[k], recv_sem=recv_sem.at[k],
            device_id={"rows": partner}, device_id_type=MESH,
        )
        copy.start()
        return copy

    key_mask = mask_ref[...].astype(F32)
    lane = iota((1, res), 1)
    row_mask = [
        jnp.sum(jnp.where(lane == me * rows + r, key_mask, 0.0), axis=1, keepdims=True) for r in range(rows)
    ]
    spreads = [spread_rows(2 * cz, cz, r) for r in range(2)]
    pair_send[...] = pair_ref[...].reshape(rows, n, 2, cz)
    normed = jnp.concatenate(
        [norm_lanes(pair_ref[r].astype(F32)).astype(BF) for r in range(rows)], axis=1
    )

    def projected(g):
        w = w_in_ref[:, g * cz : (g + 1) * cz]
        spread_w = jnp.concatenate([dot(s, w, NT).astype(BF) for s in spreads], axis=1)
        return dot(spread_w, normed, NT)

    parity = iota((2 * cz, res), 0) % 2
    pair_mask = jnp.where(parity == 0, row_mask[0], row_mask[1]) * key_mask
    for a in range(2):
        edge = (sigmoid(projected(2 * a)) * projected(2 * a + 1) * pair_mask).astype(BF)
        edge_send[:, a] = edge.reshape(n, 2, res)

    pl.semaphore_wait(barrier, n - 1)
    exchange(lambda d: edge_send.at[d], edge_recv.at[me], 0)
    exchange(lambda d: pair_send.at[:, d], pair_recv.at[me], 1)

    whole_wait(edge_recv, recv_sem.at[0])
    left = edge_recv[:, 0].reshape(res, res)
    right = edge_recv[:, 1].reshape(res, res)
    prod_send[...] = dot(right, left, NT).astype(BF).reshape(n, 2, res)
    exchange(lambda d: prod_send.at[d], prod_recv.at[me], 2)

    whole_wait(pair_recv, recv_sem.at[1])
    tokens[...] = pair_recv[...].reshape(2 * res, cz).astype(F32)
    columns = [tokens[pl.ds(jj, res, stride=2), :] for jj in range(2)]
    gates = [sigmoid(dot(norm_lanes(x).astype(BF), w_tg_ref[...])) for x in columns]
    w_to = w_to_ref[...]
    spread_out = jnp.concatenate([dot(s, w_to).astype(BF) for s in spreads], axis=1)
    e_row = iota((8, HEADS), 0)
    e_col = iota((8, HEADS), 1)
    w_bias = jnp.concatenate(
        [
            dot(((e_row // 2 == e_col) & (e_row % 2 == jj)).astype(F32).astype(BF), w_ab_ref[...], NT).astype(BF)
            for jj in range(2)
        ],
        axis=1,
    )

    whole_wait(prod_recv, recv_sem.at[2])
    product = prod_recv[...].reshape(2 * cz, res).astype(F32)
    sub = iota((8, res), 0) % 2

    def column_mean(x):
        total = jnp.sum(x.reshape(2 * cz // 8, 8, res), axis=0)
        even = jnp.sum(jnp.where(sub == 0, total, 0.0), axis=0, keepdims=True)
        odd = jnp.sum(jnp.where(sub == 0, 0.0, total), axis=0, keepdims=True)
        return jnp.where(sub == 0, even, odd) * (1.0 / cz)

    tall = product.reshape(2 * cz // 8, 8, res)
    tall = tall - column_mean(product)[None]
    spread = column_mean((tall * tall).reshape(2 * cz, res))
    tri = (tall * lax.rsqrt(spread + EPSILON)[None]).reshape(2 * cz, res).astype(BF)
    update = dot(tri, spread_out, TN)
    for jj in range(2):
        mid = (columns[jj] + gates[jj] * update[:, jj * cz : (jj + 1) * cz]).astype(BF).astype(F32)
        middle[jj] = mid
        att_own[jj] = norm_lanes(mid).astype(BF)
    to_partner(att_own, att_peer, 4)
    both = jnp.concatenate([att_own[0], att_own[1]], axis=1)
    bias_send[...] = dot(w_bias, both, NT).reshape(2, 4, res)
    exchange(lambda d: bias_send.at[lax.rem(d, 2)], bias_recv.at[me], 3)

    penalty = (key_mask - 1.0) * MASK_PENALTY
    lane_head = iota((1, cz), 1) // HEAD_DIM
    head_mask = [lane_head == 2 * core + h for h in range(2)]
    values = []
    for l in range(4):
        if l == 2:
            whole_wait(att_peer, recv_sem.at[4])
        x = att_own[l] if l < 2 else att_peer[l - 2]
        qkv = dot(x, w_qkv_ref[...]).astype(BF)
        for h in range(2):
            key = jnp.where(head_mask[h], qkv[:, cz : 2 * cz], 0)
            scores[2 * l + h] = dot(qkv[:, :cz], key, NT) * (HEAD_DIM ** -0.5) + penalty
        values.append(qkv[:, 2 * cz :])
    att_gates = [sigmoid(dot(att_own[jj], w_ag_ref[...])) for jj in range(2)]

    whole_wait(bias_recv, recv_sem.at[3])
    any_head = head_mask[0] | head_mask[1]

    def attended(l):
        total = None
        for h in range(2):
            s = scores[2 * l + h] + bias_recv[:, 2 * h : 2 * h + 2].reshape(res, res)
            e = jnp.exp(s - jnp.max(s, axis=1, keepdims=True)).astype(BF)
            ones = jnp.broadcast_to(jnp.where(head_mask[h], 1.0, 0.0), (res, cz)).astype(BF)
            part = dot(e, jnp.concatenate([jnp.where(head_mask[h], values[l], 0), ones], axis=1))
            total = part if total is None else total + part
        return (total[:, :cz] / jnp.where(any_head, total[:, cz:], 1.0)).astype(BF)

    for l in (2, 3):
        o_send[l - 2] = attended(l)
        to_partner(o_send.at[l - 2], o_recv.at[l - 2], 3 + l)
    for jj in range(2):
        o_own[jj] = attended(jj)
    for jj in range(2):
        whole_wait(o_recv.at[jj], recv_sem.at[5 + jj])
        att = o_own[jj].astype(F32) + o_recv[jj].astype(F32)
        gated = (att_gates[jj] * att).astype(BF)
        tokens[pl.ds(jj, res, stride=2), :] = middle[jj] + dot(gated, w_ao_ref[...])
    upd_send[...] = tokens[...].astype(BF).reshape(n, rows, 2, cz)
    exchange(lambda d: upd_send.at[d], upd_recv.at[:, me], 7)
    whole_wait(upd_recv, recv_sem.at[7])
    out_ref[...] = upd_recv[...].reshape(rows, res, cz)

    others = pl.ds(0, n - 1)
    whole_wait(edge_recv.at[others], send_sem.at[0])
    whole_wait(pair_recv.at[others], send_sem.at[1])
    whole_wait(prod_recv.at[others], send_sem.at[2])
    whole_wait(bias_recv.at[others], send_sem.at[3])
    whole_wait(att_peer, send_sem.at[4])
    whole_wait(o_recv.at[0], send_sem.at[5])
    whole_wait(o_recv.at[1], send_sem.at[6])
    whole_wait(upd_recv.at[:, others], send_sem.at[7])


def local(n, pair, mask, w_tri_in, w_tri_gate, w_tri_out, w_qkv, w_att_bias, w_att_gate, w_att_out):
    rows, res, cz = pair.shape
    vmem = pl.BlockSpec(memory_space=pltpu.VMEM)
    return pl.pallas_call(
        functools.partial(kernel, n),
        out_shape=jax.ShapeDtypeStruct(pair.shape, BF),
        in_specs=[vmem] * 9,
        out_specs=vmem,
        scratch_shapes=[
            pltpu.VMEM((rows, n, 2, cz), BF),
            pltpu.VMEM((n, 2, 2, res), BF),
            pltpu.VMEM((n, 2, 2, res), BF),
            pltpu.VMEM((n, rows, 2, cz), BF),
            pltpu.VMEM((n, 2, res), BF),
            pltpu.VMEM((n, 2, res), BF),
            pltpu.VMEM((2 * res, cz), F32),
            pltpu.VMEM((2, res, cz), F32),
            pltpu.VMEM((2, res, cz), BF),
            pltpu.VMEM((2, res, cz), BF),
            pltpu.VMEM((2, 4, res), F32),
            pltpu.VMEM((n, 4, res), F32),
            pltpu.VMEM((8, res, res), F32),
            pltpu.VMEM((2, res, cz), BF),
            pltpu.VMEM((2, res, cz), BF),
            pltpu.VMEM((2, res, cz), BF),
            pltpu.VMEM((n, rows, 2, cz), BF),
            pltpu.VMEM((rows, n, 2, cz), BF),
            pltpu.SemaphoreType.DMA((8,)),
            pltpu.SemaphoreType.DMA((8,)),
        ],
        compiler_params=pltpu.CompilerParams(collective_id=0, has_side_effects=True),
        name="pair_update",
    )(pair, mask.reshape(1, res), w_tri_in, w_tri_gate, w_tri_out, w_qkv, w_att_bias, w_att_gate, w_att_out)


def solution(mesh):
    split = P(("parts", "rows"), None, None)
    placed = (split, P("parts"), P(), P(), P(), P(), P(), P(), P())
    return jax.shard_map(
        functools.partial(local, mesh.shape["rows"]), mesh=mesh, in_specs=placed, out_specs=split, check_vma=False
    )
```

```python
import functools
import math
import random

import jax
import jax.numpy as jnp
from jax import lax
from jax.experimental import pallas as pl
from jax.experimental.pallas import tpu as pltpu
from jax.sharding import PartitionSpec as P

HEADS = 4
HEAD_DIM = 32
EPSILON = 1e-05
MASK_PENALTY = 1000000000.0
MESH = pl.DeviceIdType.MESH
BF = jnp.bfloat16
F32 = jnp.float32
NN = (((1,), (0,)), ((), ()))
NT = (((1,), (1,)), ((), ()))
TN = (((0,), (0,)), ((), ()))

def far_first(side):
    order = [(x, y, c) for x in range(side) for y in range(side) for c in range(2) if x + y + c]
    random.Random(1).shuffle(order)
    return sorted(order, key=lambda o: -(min(o[0], side - o[0]) + min(o[1], side - o[1])))

def dot(a, b, dims=NN):
    return lax.dot_general(a, b, dims, preferred_element_type=F32)

def sigmoid(x):
    return 0.5 * jnp.tanh(0.5 * x) + 0.5

def norm_lanes(x):
    center = jnp.mean(x, axis=1, keepdims=True)
    shifted = x - center
    spread = jnp.mean(shifted * shifted, axis=1, keepdims=True)
    return shifted * lax.rsqrt(spread + EPSILON)

def iota(shape, dim):
    return lax.broadcasted_iota(jnp.int32, shape, dim)

def spread_rows(rows, picked, parity):
    return (iota((rows, picked), 0) == 2 * iota((rows, picked), 1) + parity).astype(F32).astype(BF)

def whole_wait(ref, sem):
    pltpu.make_async_copy(ref, ref, sem).wait()

def kernel(
    n,
    pair_hbm, mask_hbm, w_in_hbm, w_tg_hbm, w_to_hbm, w_qkv_hbm, w_ab_hbm, w_ag_hbm, w_ao_hbm,
    out_ref,
    pair_ref, mask_ref, w_in_ref, w_tg_ref, w_to_ref, w_qkv_ref, w_ab_ref, w_ag_ref, w_ao_ref,
    pair_send, pair_mid, pair_recv, edge_send, edge_mid, edge_recv, prod_send, prod_recv,
    tokens, middle, att_own, att_peer, bias_send, bias_recv, scores, o_send, o_recv, o_own, upd_send, upd_recv,
    load_sem, send_sem, recv_sem, edge_sem, pair_sem, bias_sem,
):
    loads = [
        pltpu.make_async_copy(hbm, ref, load_sem.at[i])
        for i, (hbm, ref) in enumerate(
            zip(
                (pair_hbm, mask_hbm, w_in_hbm, w_tg_hbm, w_to_hbm, w_qkv_hbm, w_ab_hbm, w_ag_hbm, w_ao_hbm),
                (pair_ref, mask_ref, w_in_ref, w_tg_ref, w_to_ref, w_qkv_ref, w_ab_ref, w_ag_ref, w_ao_ref),
            )
        )
    ]
    for load in loads:
        load.start()
    rows, res, cz = pair_ref.shape
    side = math.isqrt(n // 2)
    me = lax.axis_index("rows")
    core = lax.rem(me, 2)
    x = me // (2 * side)
    y = lax.rem(me // 2, side)
    partner = me + 1 - 2 * core
    lead = x + core * (y - x)
    far = sorted(range(1, side), key=lambda t: -min(t, side - t))
    near = sorted(range(1, side), key=lambda t: min(t, side - t))

    def chip(tx, ty):
        return lax.rem(x + tx, side) * side + lax.rem(y + ty, side)

    barrier = pltpu.get_barrier_semaphore()

    def greet(device):
        pl.semaphore_signal(barrier, inc=1, device_id={"rows": device}, device_id_type=MESH)

    for t in far:
        for c in range(2):
            greet(2 * chip(t, 0) + c)
            greet(2 * chip(0, t) + c)
    greet(partner)

    def push(source, target, sent, received, device):
        copy = pltpu.make_async_remote_copy(
            src_ref=source, dst_ref=target, send_sem=send_sem.at[sent], recv_sem=received,
            device_id={"rows": device}, device_id_type=MESH,
        )
        copy.start()

    def first_leg(send_ref, mid_ref, sent, sems):
        @pl.when(core == 0)
        def _():
            for t in far:
                push(
                    send_ref.at[lax.rem(x + t, side)], mid_ref.at[x], sent, sems.at[(side - t) % side],
                    2 * chip(t, 0),
                )

        @pl.when(core == 1)
        def _():
            for t in far:
                push(
                    send_ref.at[:, lax.rem(y + t, side)], mid_ref.at[y], sent, sems.at[(side - t) % side],
                    2 * chip(0, t) + 1,
                )

    def second_leg(send_ref, mid_ref, recv_ref, sent, sems, received):
        for u in [0] + near:
            s = lax.rem(lead + u, side)
            if u:
                whole_wait(mid_ref.at[s], sems.at[u])
            origin = (s + core * (x - s)) * 2 * side + (y + core * (s - y)) * 2 + core
            for t in far + [0]:
                tx, ty = core * t, (1 - core) * t
                across = lax.rem(y + core * (x - y) + t, side)
                for dc in range(2):
                    c = core + dc - 2 * core * dc
                    if u:
                        source = mid_ref.at[s, across, c]
                    else:
                        source = send_ref.at[lax.rem(x + tx, side), lax.rem(y + ty, side), c]
                    if t or dc:
                        push(source, recv_ref.at[origin], sent, received, 2 * chip(tx, ty) + c)
                    else:
                        pltpu.make_async_copy(source, recv_ref.at[origin], received).start()

    def exchange(source, target, k):
        for tx, ty, tc in far_first(side):
            d = 2 * chip(tx, ty) + core + tc - 2 * core * tc
            push(source(d), target, k, recv_sem.at[k], d)
        pltpu.make_async_copy(source(me), target, recv_sem.at[k]).start()

    def to_partner(source, target, k):
        push(source, target, k, recv_sem.at[k], partner)

    for load in loads:
        load.wait()

    key_mask = mask_ref[...].astype(F32)
    lane = iota((1, res), 1)
    row_mask = [
        jnp.sum(jnp.where(lane == me * rows + r, key_mask, 0.0), axis=1, keepdims=True) for r in range(rows)
    ]
    spreads = [spread_rows(2 * cz, cz, r) for r in range(2)]
    for r in range(rows):
        pair_send[:, :, :, r] = pair_ref[r].reshape(side, side, 2, 2, cz)
    normed = jnp.concatenate(
        [norm_lanes(pair_ref[r].astype(F32)).astype(BF) for r in range(rows)], axis=1
    )

    def projected(g):
        w = w_in_ref[:, g * cz : (g + 1) * cz]
        spread_w = jnp.concatenate([dot(s, w, NT).astype(BF) for s in spreads], axis=1)
        return dot(spread_w, normed, NT)

    parity = iota((2 * cz, res), 0) % 2
    pair_mask = jnp.where(parity == 0, row_mask[0], row_mask[1]) * key_mask
    for a in range(2):
        edge = (sigmoid(projected(2 * a)) * projected(2 * a + 1) * pair_mask).astype(BF)
        edge_send[:, :, :, a] = edge.reshape(side, side, 2, 2, res)

    pl.semaphore_wait(barrier, 4 * side - 3)
    first_leg(edge_send, edge_mid, 8, edge_sem)
    first_leg(pair_send, pair_mid, 9, pair_sem)
    second_leg(edge_send, edge_mid, edge_recv, 0, edge_sem, recv_sem.at[0])
    second_leg(pair_send, pair_mid, pair_recv, 1, pair_sem, recv_sem.at[1])

    whole_wait(edge_recv, recv_sem.at[0])
    left = edge_recv[:, 0].reshape(res, res)
    right = edge_recv[:, 1].reshape(res, res)
    prod_send[...] = dot(right, left, NT).astype(BF).reshape(n, 2, res)
    exchange(lambda d: prod_send.at[d], prod_recv.at[me], 2)

    whole_wait(pair_recv, recv_sem.at[1])
    tokens[...] = pair_recv[...].reshape(2 * res, cz).astype(F32)
    columns = [tokens[pl.ds(jj, res, stride=2), :] for jj in range(2)]
    gates = [sigmoid(dot(norm_lanes(x).astype(BF), w_tg_ref[...])) for x in columns]
    w_to = w_to_ref[...]
    spread_out = jnp.concatenate([dot(s, w_to).astype(BF) for s in spreads], axis=1)
    e_row = iota((8, HEADS), 0)
    e_col = iota((8, HEADS), 1)
    w_bias = jnp.concatenate(
        [
            dot(((e_row // 2 == e_col) & (e_row % 2 == jj)).astype(F32).astype(BF), w_ab_ref[...], NT).astype(BF)
            for jj in range(2)
        ],
        axis=1,
    )

    whole_wait(prod_recv, recv_sem.at[2])
    product = prod_recv[...].reshape(2 * cz, res).astype(F32)
    sub = iota((8, res), 0) % 2

    def column_mean(x):
        total = jnp.sum(x.reshape(2 * cz // 8, 8, res), axis=0)
        even = jnp.sum(jnp.where(sub == 0, total, 0.0), axis=0, keepdims=True)
        odd = jnp.sum(jnp.where(sub == 0, 0.0, total), axis=0, keepdims=True)
        return jnp.where(sub == 0, even, odd) * (1.0 / cz)

    tall = product.reshape(2 * cz // 8, 8, res)
    tall = tall - column_mean(product)[None]
    spread = column_mean((tall * tall).reshape(2 * cz, res))
    tri = (tall * lax.rsqrt(spread + EPSILON)[None]).reshape(2 * cz, res).astype(BF)
    update = dot(tri, spread_out, TN)
    for jj in range(2):
        mid = (columns[jj] + gates[jj] * update[:, jj * cz : (jj + 1) * cz]).astype(BF).astype(F32)
        middle[jj] = mid
        att_own[jj] = norm_lanes(mid).astype(BF)
    to_partner(att_own, att_peer, 4)
    both = jnp.concatenate([att_own[0], att_own[1]], axis=1)
    bias_send[...] = dot(w_bias, both, NT).reshape(2, 4, res)
    for t in far:
        push(bias_send.at[0], bias_recv.at[me], 3, bias_sem.at[(side - t) % side], 2 * chip(t, 0))
        push(bias_send.at[1], bias_recv.at[me], 3, bias_sem.at[(side - t) % side], 2 * chip(0, t) + 1)
    push(bias_send.at[1 - core], bias_recv.at[me], 3, bias_sem.at[0], partner)
    pltpu.make_async_copy(bias_send.at[core], bias_recv.at[me], bias_sem.at[0]).start()

    def pass_on(u):
        s = lax.rem(lead + u, side)
        block = bias_recv.at[pl.ds(2 * ((s + core * (x - s)) * side + y + core * (s - y)), 2)]
        whole_wait(block, bias_sem.at[u])
        for t in far:
            push(block, block, 10, recv_sem.at[3], 2 * chip(core * t, (1 - core) * t) + core)

    penalty = (key_mask - 1.0) * MASK_PENALTY
    lane_head = iota((1, cz), 1) // HEAD_DIM
    head_mask = [lane_head == 2 * core + h for h in range(2)]
    values = []

    def score(rows_in):
        qkv = dot(rows_in, w_qkv_ref[...]).astype(BF)
        for h in range(2):
            key = jnp.where(head_mask[h], qkv[:, cz : 2 * cz], 0)
            scores[2 * len(values) + h] = dot(qkv[:, :cz], key, NT) * (HEAD_DIM ** -0.5) + penalty
        values.append(qkv[:, 2 * cz :])

    score(att_own[0])
    pass_on(0)
    score(att_own[1])
    whole_wait(att_peer, recv_sem.at[4])
    pass_on(near[0])
    pass_on(near[1])
    score(att_peer[0])
    pass_on(near[2])
    pass_on(near[3])
    score(att_peer[1])
    for u in near[4:]:
        pass_on(u)
    att_gates = [sigmoid(dot(att_own[jj], w_ag_ref[...])) for jj in range(2)]

    whole_wait(bias_recv.at[pl.ds(0, n - 2 * side)], recv_sem.at[3])
    any_head = head_mask[0] | head_mask[1]

    def attended(l):
        total = None
        for h in range(2):
            s = scores[2 * l + h] + bias_recv[:, 2 * h : 2 * h + 2].reshape(res, res)
            e = jnp.exp(s - jnp.max(s, axis=1, keepdims=True)).astype(BF)
            ones = jnp.broadcast_to(jnp.where(head_mask[h], 1.0, 0.0), (res, cz)).astype(BF)
            part = dot(e, jnp.concatenate([jnp.where(head_mask[h], values[l], 0), ones], axis=1))
            total = part if total is None else total + part
        return (total[:, :cz] / jnp.where(any_head, total[:, cz:], 1.0)).astype(BF)

    for l in (2, 3):
        o_send[l - 2] = attended(l)
        to_partner(o_send.at[l - 2], o_recv.at[l - 2], 3 + l)
    for jj in range(2):
        o_own[jj] = attended(jj)
    for jj in range(2):
        whole_wait(o_recv.at[jj], recv_sem.at[5 + jj])
        att = o_own[jj].astype(F32) + o_recv[jj].astype(F32)
        gated = (att_gates[jj] * att).astype(BF)
        tokens[pl.ds(jj, res, stride=2), :] = middle[jj] + dot(gated, w_ao_ref[...])
    upd_send[...] = tokens[...].astype(BF).reshape(n, rows, 2, cz)
    exchange(lambda d: upd_send.at[d], upd_recv.at[:, me], 7)
    whole_wait(upd_recv, recv_sem.at[7])
    out_ref[...] = upd_recv[...].reshape(rows, res, cz)

    others = pl.ds(0, n - 1)
    passed = pl.ds(0, n - side)
    whole_wait(edge_recv.at[passed], send_sem.at[0])
    whole_wait(pair_recv.at[passed], send_sem.at[1])
    whole_wait(prod_recv.at[others], send_sem.at[2])
    whole_wait(bias_recv.at[pl.ds(0, 2 * side - 1)], send_sem.at[3])
    whole_wait(att_peer, send_sem.at[4])
    whole_wait(o_recv.at[0], send_sem.at[5])
    whole_wait(o_recv.at[1], send_sem.at[6])
    whole_wait(upd_recv.at[:, others], send_sem.at[7])
    whole_wait(edge_mid.at[pl.ds(0, side - 1)], send_sem.at[8])
    whole_wait(pair_mid.at[pl.ds(0, side - 1)], send_sem.at[9])
    whole_wait(bias_recv.at[pl.ds(0, n - 2 * side)], send_sem.at[10])

def local(n, *args):
    args = [args[0], args[1].reshape(1, -1), *args[2:]]
    rows, res, cz = args[0].shape
    side = math.isqrt(n // 2)
    pair_grid = (side, side, 2, rows, 2, cz)
    edge_grid = (side, side, 2, 2, 2, res)
    return pl.pallas_call(
        functools.partial(kernel, n),
        out_shape=jax.ShapeDtypeStruct(args[0].shape, BF),
        in_specs=[pl.BlockSpec(memory_space=pl.ANY)] * len(args),
        out_specs=pl.BlockSpec(memory_space=pltpu.VMEM),
        scratch_shapes=[pltpu.VMEM(a.shape, a.dtype) for a in args]
        + [
            pltpu.VMEM(pair_grid, BF),
            pltpu.VMEM(pair_grid, BF),
            pltpu.VMEM((n, rows, 2, cz), BF),
            pltpu.VMEM(edge_grid, BF),
            pltpu.VMEM(edge_grid, BF),
            pltpu.VMEM((n, 2, 2, res), BF),
            pltpu.VMEM((n, 2, res), BF),
            pltpu.VMEM((n, 2, res), BF),
            pltpu.VMEM((2 * res, cz), F32),
            pltpu.VMEM((2, res, cz), F32),
            pltpu.VMEM((2, res, cz), BF),
            pltpu.VMEM((2, res, cz), BF),
            pltpu.VMEM((2, 4, res), F32),
            pltpu.VMEM((n, 4, res), F32),
            pltpu.VMEM((8, res, res), F32),
            pltpu.VMEM((2, res, cz), BF),
            pltpu.VMEM((2, res, cz), BF),
            pltpu.VMEM((2, res, cz), BF),
            pltpu.VMEM((n, rows, 2, cz), BF),
            pltpu.VMEM((rows, n, 2, cz), BF),
            pltpu.SemaphoreType.DMA((len(args),)),
            pltpu.SemaphoreType.DMA((11,)),
            pltpu.SemaphoreType.DMA((8,)),
            pltpu.SemaphoreType.DMA((side,)),
            pltpu.SemaphoreType.DMA((side,)),
            pltpu.SemaphoreType.DMA((side,)),
        ],
        compiler_params=pltpu.CompilerParams(collective_id=0, has_side_effects=True),
        name="pair_update",
    )(*args)

def solution(mesh):
    split = P(("parts", "rows"), None, None)
    placed = (split, P("parts"), P(), P(), P(), P(), P(), P(), P())
    return jax.shard_map(
        functools.partial(local, mesh.shape["rows"]), mesh=mesh, in_specs=placed, out_specs=split, check_vma=False
    )
```

```python
import functools
import math
import random

import jax
import jax.numpy as jnp
from jax import lax
from jax.experimental import pallas as pl
from jax.experimental.pallas import tpu as pltpu
from jax.sharding import PartitionSpec as P

HEADS = 4
HEAD_DIM = 32
EPSILON = 1e-05
MASK_PENALTY = 1000000000.0
MESH = pl.DeviceIdType.MESH
BF = jnp.bfloat16
F32 = jnp.float32
NN = (((1,), (0,)), ((), ()))
NT = (((1,), (1,)), ((), ()))
TN = (((0,), (0,)), ((), ()))

def far_first(side):
    order = [(x, y, c) for x in range(side) for y in range(side) for c in range(2) if x + y + c]
    random.Random(1).shuffle(order)
    return sorted(order, key=lambda o: -(min(o[0], side - o[0]) + min(o[1], side - o[1])))

def dot(a, b, dims=NN):
    return lax.dot_general(a, b, dims, preferred_element_type=F32)

def sigmoid(x):
    return 0.5 * jnp.tanh(0.5 * x) + 0.5

def norm_lanes(x):
    center = jnp.mean(x, axis=1, keepdims=True)
    shifted = x - center
    spread = jnp.mean(shifted * shifted, axis=1, keepdims=True)
    return shifted * lax.rsqrt(spread + EPSILON)

def iota(shape, dim):
    return lax.broadcasted_iota(jnp.int32, shape, dim)

def spread_rows(rows, picked, parity):
    return (iota((rows, picked), 0) == 2 * iota((rows, picked), 1) + parity).astype(F32).astype(BF)

def whole_wait(ref, sem):
    pltpu.make_async_copy(ref, ref, sem).wait()

def kernel(
    n,
    pair_hbm, mask_hbm, w_in_hbm, w_tg_hbm, w_to_hbm, w_qkv_hbm, w_ab_hbm, w_ag_hbm, w_ao_hbm,
    out_ref,
    pair_ref, mask_ref, w_in_ref, w_tg_ref, w_to_ref, w_qkv_ref, w_ab_ref, w_ag_ref, w_ao_ref,
    pair_send, pair_mid, pair_recv, edge_send, edge_mid, edge_recv, prod_send, prod_recv,
    tokens, middle, att_own, att_peer, bias_send, bias_recv, scores, o_send, o_recv, o_own, upd_send, upd_recv,
    load_sem, send_sem, recv_sem, edge_sem, pair_sem, bias_sem, ready_sem, late_sem,
):
    loads = [
        pltpu.make_async_copy(hbm, ref, load_sem.at[i])
        for i, (hbm, ref) in enumerate(
            zip(
                (pair_hbm, mask_hbm, w_in_hbm, w_tg_hbm, w_to_hbm, w_qkv_hbm, w_ab_hbm, w_ag_hbm, w_ao_hbm),
                (pair_ref, mask_ref, w_in_ref, w_tg_ref, w_to_ref, w_qkv_ref, w_ab_ref, w_ag_ref, w_ao_ref),
            )
        )
    ]
    for load in loads:
        load.start()
    rows, res, cz = pair_ref.shape
    side = math.isqrt(n // 2)
    me = lax.axis_index("rows")
    core = lax.rem(me, 2)
    x = me // (2 * side)
    y = lax.rem(me // 2, side)
    partner = me + 1 - 2 * core
    lead = x + core * (y - x)
    far = sorted(range(1, side), key=lambda t: -min(t, side - t))
    near = sorted(range(1, side), key=lambda t: min(t, side - t))

    def chip(tx, ty):
        return lax.rem(x + tx, side) * side + lax.rem(y + ty, side)

    barrier = pltpu.get_barrier_semaphore()

    def greet(device):
        pl.semaphore_signal(barrier, inc=1, device_id={"rows": device}, device_id_type=MESH)

    first = me == 0
    beside_first = me == 1
    in_row = (y == 0) & (x > 0)
    in_column = (x == 0) & (y > 0)
    feeds_first = in_row & (core == 0)
    ends_at_first = (in_column & (core == 0)) | (in_row & (core == 1))

    @pl.when(me > 0)
    def _():
        for t in far:
            greet(2 * chip(t, 0))
            greet(2 * chip(0, t) + 1)
        greet(partner)

    def tell(sem, device):
        pl.semaphore_signal(sem, inc=1, device_id={"rows": device}, device_id_type=MESH)

    @pl.when(first)
    def _():
        pl.semaphore_wait(barrier, 2 * side - 1)
        tell(ready_sem, 1)
        for t in far:
            for c in range(2):
                tell(late_sem, 2 * side * t + c)

    def push(source, target, sent, received, device):
        copy = pltpu.make_async_remote_copy(
            src_ref=source, dst_ref=target, send_sem=send_sem.at[sent], recv_sem=received,
            device_id={"rows": device}, device_id_type=MESH,
        )
        copy.start()

    def first_leg(send_ref, mid_ref, sent, sems):
        @pl.when(core == 0)
        def _():
            for t in far:
                target = lax.rem(x + t, side)

                @pl.when((y > 0) | (target > 0))
                def _():
                    push(
                        send_ref.at[target], mid_ref.at[x], sent, sems.at[(side - t) % side],
                        2 * (target * side + y),
                    )

        @pl.when(core == 1)
        def _():
            for t in far:
                push(
                    send_ref.at[:, lax.rem(y + t, side)], mid_ref.at[y], sent, sems.at[(side - t) % side],
                    2 * chip(0, t) + 1,
                )

    def first_leg_late(send_ref, mid_ref, sent, sems):
        push(send_ref.at[0], mid_ref.at[x], sent, sems.at[x], 0)

    late_u = jnp.where(feeds_first, side - x, side // 2)

    def offset(k):
        u = lax.rem(side + jnp.where(lax.rem(k, 2) == 1, (k + 1) // 2, -(k // 2)), side)
        u = jnp.where(u == late_u, side // 2, u)
        return jnp.where(k == side - 1, late_u, u)

    def origin_of(s):
        return (s + core * (x - s)) * 2 * side + (y + core * (s - y)) * 2 + core

    def second_leg(k, u, send_ref, mid_ref, recv_ref, sent, sems, received):
        s = lax.rem(lead + u, side)
        if k is not None:
            whole_wait(mid_ref.at[s], sems.at[u])
        for t in far + [0]:
            tx, ty = core * t, (1 - core) * t
            across = lax.rem(y + core * (x - y) + t, side)
            for dc in range(2):
                c = core + dc - 2 * core * dc
                if k is not None:
                    source = mid_ref.at[s, across, c]
                else:
                    source = send_ref.at[lax.rem(x + tx, side), lax.rem(y + ty, side), c]
                if t:
                    device = 2 * chip(tx, ty) + c

                    @pl.when(device > 0)
                    def _():
                        push(source, recv_ref.at[origin_of(s)], sent, received, device)
                elif dc:
                    push(source, recv_ref.at[origin_of(s)], sent, received, partner)
                else:
                    pltpu.make_async_copy(source, recv_ref.at[origin_of(s)], received).start()

    def second_leg_late(send_ref, mid_ref, recv_ref, sent, received):
        push(send_ref.at[0, 0, 0], recv_ref.at[me], sent, received, 0)
        for u in range(1, side):
            s = lax.rem(lead + u, side)
            push(mid_ref.at[s, 0, 0], recv_ref.at[origin_of(s)], sent, received, 0)

    def second_legs(*refs):
        second_leg(None, 0, *refs)

        def step(k, carry):
            second_leg(k, offset(k), *refs)
            return carry

        lax.fori_loop(1, side - 1, step, 0)

    def exchange(source, target, k):
        for tx, ty, tc in far_first(side):
            d = 2 * chip(tx, ty) + core + tc - 2 * core * tc
            push(source(d), target, k, recv_sem.at[k], d)
        pltpu.make_async_copy(source(me), target, recv_sem.at[k]).start()

    def to_partner(source, target, k):
        push(source, target, k, recv_sem.at[k], partner)

    for load in loads:
        load.wait()

    key_mask = mask_ref[...].astype(F32)
    lane = iota((1, res), 1)
    row_mask = [
        jnp.sum(jnp.where(lane == me * rows + r, key_mask, 0.0), axis=1, keepdims=True) for r in range(rows)
    ]
    spreads = [spread_rows(2 * cz, cz, r) for r in range(2)]
    for r in range(rows):
        pair_send[:, :, :, r] = pair_ref[r].reshape(side, side, 2, 2, cz)
    normed = jnp.concatenate(
        [norm_lanes(pair_ref[r].astype(F32)).astype(BF) for r in range(rows)], axis=1
    )

    def projected(g):
        w = w_in_ref[:, g * cz : (g + 1) * cz]
        spread_w = jnp.concatenate([dot(s, w, NT).astype(BF) for s in spreads], axis=1)
        return dot(spread_w, normed, NT)

    parity = iota((2 * cz, res), 0) % 2
    pair_mask = jnp.where(parity == 0, row_mask[0], row_mask[1]) * key_mask
    for a in range(2):
        edge = (sigmoid(projected(2 * a)) * projected(2 * a + 1) * pair_mask).astype(BF)
        edge_send[:, :, :, a] = edge.reshape(side, side, 2, 2, res)

    @pl.when(me > 0)
    def _():
        absent = feeds_first | ((x == 0) & (core == 1))
        pl.semaphore_wait(barrier, 2 * side - 1 - absent.astype(jnp.int32))

        @pl.when(me > 1)
        def _():
            tell(ready_sem, partner)

    edge_legs = (edge_send, edge_mid, edge_recv, 0, edge_sem, recv_sem.at[0])
    pair_legs = (pair_send, pair_mid, pair_recv, 1, pair_sem, recv_sem.at[1])
    first_leg(edge_send, edge_mid, 8, edge_sem)
    pl.semaphore_wait(ready_sem, 1)

    @pl.when(beside_first)
    def _():
        tell(ready_sem, 0)

    @pl.when(first)
    def _():
        for t in far:
            tell(late_sem, 2 * t)

    second_legs(*edge_legs)
    first_leg(pair_send, pair_mid, 9, pair_sem)

    @pl.when(feeds_first)
    def _():
        pl.semaphore_wait(late_sem, 1)
        first_leg_late(edge_send, edge_mid, 8, edge_sem)
        first_leg_late(pair_send, pair_mid, 9, pair_sem)

    second_leg(side - 1, late_u, *edge_legs)

    @pl.when(ends_at_first)
    def _():
        pl.semaphore_wait(late_sem, 1)
        second_leg_late(edge_send, edge_mid, edge_recv, 0, recv_sem.at[0])

    whole_wait(edge_recv, recv_sem.at[0])
    left = edge_recv[:, 0].reshape(res, res)
    right = edge_recv[:, 1].reshape(res, res)
    prod_send[...] = dot(right, left, NT).astype(BF).reshape(n, 2, res)
    exchange(lambda d: prod_send.at[d], prod_recv.at[me], 2)

    second_legs(*pair_legs)
    second_leg(side - 1, late_u, *pair_legs)

    @pl.when(ends_at_first)
    def _():
        second_leg_late(pair_send, pair_mid, pair_recv, 1, recv_sem.at[1])

    whole_wait(pair_recv, recv_sem.at[1])
    tokens[...] = pair_recv[...].reshape(2 * res, cz).astype(F32)
    columns = [tokens[pl.ds(jj, res, stride=2), :] for jj in range(2)]
    gates = [sigmoid(dot(norm_lanes(x).astype(BF), w_tg_ref[...])) for x in columns]
    w_to = w_to_ref[...]
    spread_out = jnp.concatenate([dot(s, w_to).astype(BF) for s in spreads], axis=1)
    e_row = iota((8, HEADS), 0)
    e_col = iota((8, HEADS), 1)
    w_bias = jnp.concatenate(
        [
            dot(((e_row // 2 == e_col) & (e_row % 2 == jj)).astype(F32).astype(BF), w_ab_ref[...]).astype(BF)
            for jj in range(2)
        ],
        axis=1,
    )

    whole_wait(prod_recv, recv_sem.at[2])
    product = prod_recv[...].reshape(2 * cz, res).astype(F32)
    sub = iota((8, res), 0) % 2

    def column_mean(x):
        total = jnp.sum(x.reshape(2 * cz // 8, 8, res), axis=0)
        even = jnp.sum(jnp.where(sub == 0, total, 0.0), axis=0, keepdims=True)
        odd = jnp.sum(jnp.where(sub == 0, 0.0, total), axis=0, keepdims=True)
        return jnp.where(sub == 0, even, odd) * (1.0 / cz)

    tall = product.reshape(2 * cz // 8, 8, res)
    tall = tall - column_mean(product)[None]
    spread = column_mean((tall * tall).reshape(2 * cz, res))
    tri = (tall * lax.rsqrt(spread + EPSILON)[None]).reshape(2 * cz, res).astype(BF)
    update = dot(tri, spread_out, TN)
    for jj in range(2):
        mid = (columns[jj] + gates[jj] * update[:, jj * cz : (jj + 1) * cz]).astype(BF).astype(F32)
        middle[jj] = mid
        att_own[jj] = norm_lanes(mid).astype(BF)
    to_partner(att_own, att_peer, 4)
    both = jnp.concatenate([att_own[0], att_own[1]], axis=1)
    bias_send[...] = dot(w_bias, both, NT).reshape(2, 4, res)
    for t in far:
        push(bias_send.at[0], bias_recv.at[me], 3, bias_sem.at[(side - t) % side], 2 * chip(t, 0))
        push(bias_send.at[1], bias_recv.at[me], 3, bias_sem.at[(side - t) % side], 2 * chip(0, t) + 1)
    push(bias_send.at[1 - core], bias_recv.at[me], 3, bias_sem.at[0], partner)
    pltpu.make_async_copy(bias_send.at[core], bias_recv.at[me], bias_sem.at[0]).start()

    def pass_on(u):
        s = lax.rem(lead + u, side)
        block = bias_recv.at[pl.ds(2 * ((s + core * (x - s)) * side + y + core * (s - y)), 2)]
        whole_wait(block, bias_sem.at[u])
        for t in far:
            push(block, block, 10, recv_sem.at[3], 2 * chip(core * t, (1 - core) * t) + core)

    penalty = (key_mask - 1.0) * MASK_PENALTY
    lane_head = iota((1, cz), 1) // HEAD_DIM
    head_mask = [lane_head == 2 * core + h for h in range(2)]
    values = []

    def score(rows_in):
        qkv = dot(rows_in, w_qkv_ref[...]).astype(BF)
        for h in range(2):
            key = jnp.where(head_mask[h], qkv[:, cz : 2 * cz], 0)
            scores[2 * len(values) + h] = dot(qkv[:, :cz], key, NT) * (HEAD_DIM ** -0.5) + penalty
        values.append(qkv[:, 2 * cz :])

    score(att_own[0])
    pass_on(0)
    score(att_own[1])
    whole_wait(att_peer, recv_sem.at[4])
    pass_on(near[0])
    pass_on(near[1])
    score(att_peer[0])
    pass_on(near[2])
    pass_on(near[3])
    score(att_peer[1])
    for u in near[4:]:
        pass_on(u)
    att_gates = [sigmoid(dot(att_own[jj], w_ag_ref[...])) for jj in range(2)]

    whole_wait(bias_recv.at[pl.ds(0, n - 2 * side)], recv_sem.at[3])
    any_head = head_mask[0] | head_mask[1]

    def attended(l):
        total = None
        for h in range(2):
            s = scores[2 * l + h] + bias_recv[:, 2 * h : 2 * h + 2].reshape(res, res)
            e = jnp.exp(s - jnp.max(s, axis=1, keepdims=True)).astype(BF)
            ones = jnp.broadcast_to(jnp.where(head_mask[h], 1.0, 0.0), (res, cz)).astype(BF)
            part = dot(e, jnp.concatenate([jnp.where(head_mask[h], values[l], 0), ones], axis=1))
            total = part if total is None else total + part
        return (total[:, :cz] / jnp.where(any_head, total[:, cz:], 1.0)).astype(BF)

    for l in (2, 3):
        o_send[l - 2] = attended(l)
        to_partner(o_send.at[l - 2], o_recv.at[l - 2], 3 + l)
    for jj in range(2):
        o_own[jj] = attended(jj)
    for jj in range(2):
        whole_wait(o_recv.at[jj], recv_sem.at[5 + jj])
        att = o_own[jj].astype(F32) + o_recv[jj].astype(F32)
        gated = (att_gates[jj] * att).astype(BF)
        tokens[pl.ds(jj, res, stride=2), :] = middle[jj] + dot(gated, w_ao_ref[...])
    upd_send[...] = tokens[...].astype(BF).reshape(n, rows, 2, cz)
    exchange(lambda d: upd_send.at[d], upd_recv.at[:, me], 7)
    whole_wait(upd_recv, recv_sem.at[7])
    out_ref[...] = upd_recv[...].reshape(rows, res, cz)

    others = pl.ds(0, n - 1)
    passed = pl.ds(0, n - side)
    whole_wait(edge_recv.at[passed], send_sem.at[0])
    whole_wait(pair_recv.at[passed], send_sem.at[1])
    whole_wait(prod_recv.at[others], send_sem.at[2])
    whole_wait(bias_recv.at[pl.ds(0, 2 * side - 1)], send_sem.at[3])
    whole_wait(att_peer, send_sem.at[4])
    whole_wait(o_recv.at[0], send_sem.at[5])
    whole_wait(o_recv.at[1], send_sem.at[6])
    whole_wait(upd_recv.at[:, others], send_sem.at[7])
    whole_wait(edge_mid.at[pl.ds(0, side - 1)], send_sem.at[8])
    whole_wait(pair_mid.at[pl.ds(0, side - 1)], send_sem.at[9])
    whole_wait(bias_recv.at[pl.ds(0, n - 2 * side)], send_sem.at[10])

def local(n, *args):
    args = [args[0], args[1].reshape(1, -1), *args[2:6], args[6].T, *args[7:]]
    rows, res, cz = args[0].shape
    side = math.isqrt(n // 2)
    pair_grid = (side, side, 2, rows, 2, cz)
    edge_grid = (side, side, 2, 2, 2, res)
    return pl.pallas_call(
        functools.partial(kernel, n),
        out_shape=pltpu.VMEM(args[0].shape, BF),
        in_specs=[pl.BlockSpec(memory_space=pl.ANY)] * len(args),
        out_specs=pl.BlockSpec(memory_space=pltpu.VMEM),
        scratch_shapes=[pltpu.VMEM(a.shape, a.dtype) for a in args]
        + [
            pltpu.VMEM(pair_grid, BF),
            pltpu.VMEM(pair_grid, BF),
            pltpu.VMEM((n, rows, 2, cz), BF),
            pltpu.VMEM(edge_grid, BF),
            pltpu.VMEM(edge_grid, BF),
            pltpu.VMEM((n, 2, 2, res), BF),
            pltpu.VMEM((n, 2, res), BF),
            pltpu.VMEM((n, 2, res), BF),
            pltpu.VMEM((2 * res, cz), F32),
            pltpu.VMEM((2, res, cz), F32),
            pltpu.VMEM((2, res, cz), BF),
            pltpu.VMEM((2, res, cz), BF),
            pltpu.VMEM((2, 4, res), F32),
            pltpu.VMEM((n, 4, res), F32),
            pltpu.VMEM((8, res, res), F32),
            pltpu.VMEM((2, res, cz), BF),
            pltpu.VMEM((2, res, cz), BF),
            pltpu.VMEM((2, res, cz), BF),
            pltpu.VMEM((n, rows, 2, cz), BF),
            pltpu.VMEM((rows, n, 2, cz), BF),
            pltpu.SemaphoreType.DMA((len(args),)),
            pltpu.SemaphoreType.DMA((11,)),
            pltpu.SemaphoreType.DMA((8,)),
            pltpu.SemaphoreType.DMA((side,)),
            pltpu.SemaphoreType.DMA((side,)),
            pltpu.SemaphoreType.DMA((side,)),
            pltpu.SemaphoreType.REGULAR,
            pltpu.SemaphoreType.REGULAR,
        ],
        compiler_params=pltpu.CompilerParams(collective_id=0, has_side_effects=True),
        name="pair_update",
    )(*args)

def solution(mesh):
    split = P(("parts", "rows"), None, None)
    placed = (split, P("parts"), P(), P(), P(), P(), P(), P(), P())
    return jax.shard_map(
        functools.partial(local, mesh.shape["rows"]), mesh=mesh, in_specs=placed, out_specs=split, check_vma=False
    )
```

```python
import functools
import math
import random

import jax
import jax.numpy as jnp
from jax import lax
from jax.experimental import pallas as pl
from jax.experimental.pallas import tpu as pltpu
from jax.sharding import PartitionSpec as P

HEADS = 4
HEAD_DIM = 32
EPSILON = 1e-05
MASK_PENALTY = 1000000000.0
MESH = pl.DeviceIdType.MESH
BF = jnp.bfloat16
F32 = jnp.float32
NN = (((1,), (0,)), ((), ()))
NT = (((1,), (1,)), ((), ()))
TN = (((0,), (0,)), ((), ()))

def far_first(side):
    order = [(x, y, c) for x in range(side) for y in range(side) for c in range(2) if x + y + c]
    random.Random(1).shuffle(order)
    return sorted(order, key=lambda o: -(min(o[0], side - o[0]) + min(o[1], side - o[1])))

def dot(a, b, dims=NN):
    return lax.dot_general(a, b, dims, preferred_element_type=F32)

def sigmoid(x):
    return 0.5 * jnp.tanh(0.5 * x) + 0.5

def norm_lanes(x):
    center = jnp.mean(x, axis=1, keepdims=True)
    shifted = x - center
    spread = jnp.mean(shifted * shifted, axis=1, keepdims=True)
    return shifted * lax.rsqrt(spread + EPSILON)

def iota(shape, dim):
    return lax.broadcasted_iota(jnp.int32, shape, dim)

def spread_rows(rows, picked, parity):
    return (iota((rows, picked), 0) == 2 * iota((rows, picked), 1) + parity).astype(F32).astype(BF)

def whole_wait(ref, sem):
    pltpu.make_async_copy(ref, ref, sem).wait()

def kernel(
    n,
    pair_hbm, mask_hbm, w_in_hbm, w_tg_hbm, w_to_hbm, w_qkv_hbm, w_ab_hbm, w_ag_hbm, w_ao_hbm,
    out_ref,
    pair_ref, mask_ref, w_in_ref, w_tg_ref, w_to_ref, w_qkv_ref, w_ab_ref, w_ag_ref, w_ao_ref,
    pair_send, pair_mid, pair_recv, edge_send, edge_mid, edge_recv, prod_send, prod_recv,
    tokens, middle, att_own, att_peer, bias_send, bias_recv, scores, o_send, o_recv, o_own, upd_send, upd_recv,
    load_sem, send_sem, recv_sem, edge_sem, pair_sem, bias_sem, ready_sem, late_sem,
):
    loads = [
        pltpu.make_async_copy(hbm, ref, load_sem.at[i])
        for i, (hbm, ref) in enumerate(
            zip(
                (pair_hbm, mask_hbm, w_in_hbm, w_tg_hbm, w_to_hbm, w_qkv_hbm, w_ab_hbm, w_ag_hbm, w_ao_hbm),
                (pair_ref, mask_ref, w_in_ref, w_tg_ref, w_to_ref, w_qkv_ref, w_ab_ref, w_ag_ref, w_ao_ref),
            )
        )
    ]
    for load in loads:
        load.start()
    rows, res, cz = pair_ref.shape
    side = math.isqrt(n // 2)
    me = lax.axis_index("rows")
    core = lax.rem(me, 2)
    x = me // (2 * side)
    y = lax.rem(me // 2, side)
    partner = me + 1 - 2 * core
    lead = x + core * (y - x)
    far = sorted(range(1, side), key=lambda t: -min(t, side - t))
    near = sorted(range(1, side), key=lambda t: min(t, side - t))

    def chip(tx, ty):
        return lax.rem(x + tx, side) * side + lax.rem(y + ty, side)

    barrier = pltpu.get_barrier_semaphore()

    def greet(device):
        pl.semaphore_signal(barrier, inc=1, device_id={"rows": device}, device_id_type=MESH)

    first = me == 0
    beside_first = me == 1
    in_row = (y == 0) & (x > 0)
    in_column = (x == 0) & (y > 0)
    feeds_first = in_row & (core == 0)
    ends_at_first = (in_column & (core == 0)) | (in_row & (core == 1))

    @pl.when(me > 0)
    def _():
        for t in far:
            greet(2 * chip(t, 0))
            greet(2 * chip(0, t) + 1)
        greet(partner)

    def tell(sem, device):
        pl.semaphore_signal(sem, inc=1, device_id={"rows": device}, device_id_type=MESH)

    @pl.when(first)
    def _():
        pl.semaphore_wait(barrier, 2 * side - 1)
        tell(ready_sem, 1)
        for t in far:
            for c in range(2):
                tell(late_sem, 2 * side * t + c)

    def push(source, target, sent, received, device):
        copy = pltpu.make_async_remote_copy(
            src_ref=source, dst_ref=target, send_sem=send_sem.at[sent], recv_sem=received,
            device_id={"rows": device}, device_id_type=MESH,
        )
        copy.start()

    def first_leg(send_ref, mid_ref, sent, sems):
        @pl.when(core == 0)
        def _():
            for t in far:
                target = lax.rem(x + t, side)

                @pl.when((y > 0) | (target > 0))
                def _():
                    push(
                        send_ref.at[target], mid_ref.at[x], sent, sems.at[(side - t) % side],
                        2 * (target * side + y),
                    )

        @pl.when(core == 1)
        def _():
            for t in far:
                push(
                    send_ref.at[:, lax.rem(y + t, side)], mid_ref.at[y], sent, sems.at[(side - t) % side],
                    2 * chip(0, t) + 1,
                )

    def first_leg_late(send_ref, mid_ref, sent, sems):
        push(send_ref.at[0], mid_ref.at[x], sent, sems.at[x], 0)

    late_u = jnp.where(feeds_first, side - x, side // 2)

    def offset(k):
        u = lax.rem(side + jnp.where(lax.rem(k, 2) == 1, (k + 1) // 2, -(k // 2)), side)
        u = jnp.where(u == late_u, side // 2, u)
        return jnp.where(k == side - 1, late_u, u)

    def origin_of(s):
        return (s + core * (x - s)) * 2 * side + (y + core * (s - y)) * 2 + core

    def second_leg(k, u, send_ref, mid_ref, recv_ref, sent, sems, received):
        s = lax.rem(lead + u, side)
        if k is not None:
            whole_wait(mid_ref.at[s], sems.at[u])
        for t in far + [0]:
            tx, ty = core * t, (1 - core) * t
            across = lax.rem(y + core * (x - y) + t, side)
            for dc in range(2):
                c = core + dc - 2 * core * dc
                if k is not None:
                    source = mid_ref.at[s, across, c]
                else:
                    source = send_ref.at[lax.rem(x + tx, side), lax.rem(y + ty, side), c]
                if t:
                    device = 2 * chip(tx, ty) + c

                    @pl.when(device > 0)
                    def _():
                        push(source, recv_ref.at[origin_of(s)], sent, received, device)
                elif dc:
                    push(source, recv_ref.at[origin_of(s)], sent, received, partner)
                else:
                    pltpu.make_async_copy(source, recv_ref.at[origin_of(s)], received).start()

    def second_leg_late(send_ref, mid_ref, recv_ref, sent, received):
        push(send_ref.at[0, 0, 0], recv_ref.at[me], sent, received, 0)
        for u in range(1, side):
            s = lax.rem(lead + u, side)
            push(mid_ref.at[s, 0, 0], recv_ref.at[origin_of(s)], sent, received, 0)

    def second_leg_at_once(send_ref, mid_ref, recv_ref, sent, sems, received):
        @pl.when(core == 0)
        def _():
            pltpu.make_async_copy(send_ref.at[x], mid_ref.at[x], sems.at[0]).start()

        @pl.when(core == 1)
        def _():
            pltpu.make_async_copy(send_ref.at[:, y], mid_ref.at[y], sems.at[0]).start()

        for u in range(side):
            whole_wait(mid_ref.at[lax.rem(lead + u, side)], sems.at[u])
        for along in range(2):

            @pl.when(core == along)
            def _():
                target = recv_ref.at[x, :, 1] if along else recv_ref.at[:, y, 0]
                for t in far + [0]:
                    across = lax.rem((x if along else y) + t, side)
                    for c in range(2):
                        source = mid_ref.at[:, across, c]
                        if t or c != along:
                            push(source, target, sent, received, 2 * (chip(t, 0) if along else chip(0, t)) + c)
                        else:
                            pltpu.make_async_copy(source, target, received).start()

    def second_legs(*refs):
        second_leg(None, 0, *refs)

        def step(k, carry):
            second_leg(k, offset(k), *refs)
            return carry

        lax.fori_loop(1, side - 1, step, 0)

    def exchange(source, target, k):
        for tx, ty, tc in far_first(side):
            d = 2 * chip(tx, ty) + core + tc - 2 * core * tc
            push(source(d), target, k, recv_sem.at[k], d)
        pltpu.make_async_copy(source(me), target, recv_sem.at[k]).start()

    def to_partner(source, target, k):
        push(source, target, k, recv_sem.at[k], partner)

    for load in loads:
        load.wait()

    key_mask = mask_ref[...].astype(F32)
    lane = iota((1, res), 1)
    row_mask = [
        jnp.sum(jnp.where(lane == me * rows + r, key_mask, 0.0), axis=1, keepdims=True) for r in range(rows)
    ]
    spreads = [spread_rows(2 * cz, cz, r) for r in range(2)]
    for r in range(rows):
        pair_send[:, :, :, r] = pair_ref[r].reshape(side, side, 2, 2, cz)
    normed = jnp.concatenate(
        [norm_lanes(pair_ref[r].astype(F32)).astype(BF) for r in range(rows)], axis=1
    )

    def projected(g):
        w = w_in_ref[:, g * cz : (g + 1) * cz]
        spread_w = jnp.concatenate([dot(s, w, NT).astype(BF) for s in spreads], axis=1)
        return dot(spread_w, normed, NT)

    parity = iota((2 * cz, res), 0) % 2
    pair_mask = jnp.where(parity == 0, row_mask[0], row_mask[1]) * key_mask
    for a in range(2):
        edge = (sigmoid(projected(2 * a)) * projected(2 * a + 1) * pair_mask).astype(BF)
        edge_send[:, :, :, a] = edge.reshape(side, side, 2, 2, res)

    @pl.when(me > 0)
    def _():
        absent = feeds_first | ((x == 0) & (core == 1))
        pl.semaphore_wait(barrier, 2 * side - 1 - absent.astype(jnp.int32))

        @pl.when(me > 1)
        def _():
            tell(ready_sem, partner)

    edge_legs = (edge_send, edge_mid, edge_recv, 0, edge_sem, recv_sem.at[0])
    pair_legs = (pair_send, pair_mid, pair_recv, 1, pair_sem, recv_sem.at[1])
    first_leg(edge_send, edge_mid, 8, edge_sem)
    pl.semaphore_wait(ready_sem, 1)

    @pl.when(beside_first)
    def _():
        tell(ready_sem, 0)

    @pl.when(first)
    def _():
        for t in far:
            tell(late_sem, 2 * t)

    second_legs(*edge_legs)
    first_leg(pair_send, pair_mid, 9, pair_sem)

    @pl.when(feeds_first)
    def _():
        pl.semaphore_wait(late_sem, 1)
        first_leg_late(edge_send, edge_mid, 8, edge_sem)
        first_leg_late(pair_send, pair_mid, 9, pair_sem)

    second_leg(side - 1, late_u, *edge_legs)

    @pl.when(ends_at_first)
    def _():
        pl.semaphore_wait(late_sem, 1)
        second_leg_late(edge_send, edge_mid, edge_recv, 0, recv_sem.at[0])

    second_leg_at_once(*pair_legs)

    whole_wait(edge_recv, recv_sem.at[0])
    left = edge_recv[:, 0].reshape(res, res)
    right = edge_recv[:, 1].reshape(res, res)
    prod_send[...] = dot(right, left, NT).astype(BF).reshape(n, 2, res)
    exchange(lambda d: prod_send.at[d], prod_recv.at[me], 2)

    whole_wait(pair_recv, recv_sem.at[1])
    tokens[...] = pair_recv[...].reshape(2 * res, cz).astype(F32)
    columns = [tokens[pl.ds(jj, res, stride=2), :] for jj in range(2)]
    gates = [sigmoid(dot(norm_lanes(x).astype(BF), w_tg_ref[...])) for x in columns]
    w_to = w_to_ref[...]
    spread_out = jnp.concatenate([dot(s, w_to).astype(BF) for s in spreads], axis=1)
    e_row = iota((8, HEADS), 0)
    e_col = iota((8, HEADS), 1)
    w_bias = jnp.concatenate(
        [
            dot(((e_row // 2 == e_col) & (e_row % 2 == jj)).astype(F32).astype(BF), w_ab_ref[...]).astype(BF)
            for jj in range(2)
        ],
        axis=1,
    )

    whole_wait(prod_recv, recv_sem.at[2])
    product = prod_recv[...].reshape(2 * cz, res).astype(F32)
    sub = iota((8, res), 0) % 2

    def column_mean(x):
        total = jnp.sum(x.reshape(2 * cz // 8, 8, res), axis=0)
        even = jnp.sum(jnp.where(sub == 0, total, 0.0), axis=0, keepdims=True)
        odd = jnp.sum(jnp.where(sub == 0, 0.0, total), axis=0, keepdims=True)
        return jnp.where(sub == 0, even, odd) * (1.0 / cz)

    tall = product.reshape(2 * cz // 8, 8, res)
    tall = tall - column_mean(product)[None]
    spread = column_mean((tall * tall).reshape(2 * cz, res))
    tri = (tall * lax.rsqrt(spread + EPSILON)[None]).reshape(2 * cz, res).astype(BF)
    update = dot(tri, spread_out, TN)
    for jj in range(2):
        mid = (columns[jj] + gates[jj] * update[:, jj * cz : (jj + 1) * cz]).astype(BF).astype(F32)
        middle[jj] = mid
        att_own[jj] = norm_lanes(mid).astype(BF)
    to_partner(att_own, att_peer, 4)
    both = jnp.concatenate([att_own[0], att_own[1]], axis=1)
    bias_send[...] = dot(w_bias, both, NT).reshape(2, 4, res)
    for t in far:
        push(bias_send.at[0], bias_recv.at[me], 3, bias_sem.at[(side - t) % side], 2 * chip(t, 0))
        push(bias_send.at[1], bias_recv.at[me], 3, bias_sem.at[(side - t) % side], 2 * chip(0, t) + 1)
    push(bias_send.at[1 - core], bias_recv.at[me], 3, bias_sem.at[0], partner)
    pltpu.make_async_copy(bias_send.at[core], bias_recv.at[me], bias_sem.at[0]).start()

    def pass_on(u):
        s = lax.rem(lead + u, side)
        block = bias_recv.at[pl.ds(2 * ((s + core * (x - s)) * side + y + core * (s - y)), 2)]
        whole_wait(block, bias_sem.at[u])
        for t in far:
            push(block, block, 10, recv_sem.at[3], 2 * chip(core * t, (1 - core) * t) + core)

    penalty = (key_mask - 1.0) * MASK_PENALTY
    lane_head = iota((1, cz), 1) // HEAD_DIM
    head_mask = [lane_head == 2 * core + h for h in range(2)]
    values = []

    def score(rows_in):
        qkv = dot(rows_in, w_qkv_ref[...]).astype(BF)
        for h in range(2):
            key = jnp.where(head_mask[h], qkv[:, cz : 2 * cz], 0)
            scores[2 * len(values) + h] = dot(qkv[:, :cz], key, NT) * (HEAD_DIM ** -0.5) + penalty
        values.append(qkv[:, 2 * cz :])

    score(att_own[0])
    pass_on(0)
    score(att_own[1])
    whole_wait(att_peer, recv_sem.at[4])
    pass_on(near[0])
    pass_on(near[1])
    score(att_peer[0])
    pass_on(near[2])
    pass_on(near[3])
    score(att_peer[1])
    for u in near[4:]:
        pass_on(u)
    att_gates = [sigmoid(dot(att_own[jj], w_ag_ref[...])) for jj in range(2)]

    whole_wait(bias_recv.at[pl.ds(0, n - 2 * side)], recv_sem.at[3])
    any_head = head_mask[0] | head_mask[1]

    def attended(l):
        total = None
        for h in range(2):
            s = scores[2 * l + h] + bias_recv[:, 2 * h : 2 * h + 2].reshape(res, res)
            e = jnp.exp(s - jnp.max(s, axis=1, keepdims=True)).astype(BF)
            ones = jnp.broadcast_to(jnp.where(head_mask[h], 1.0, 0.0), (res, cz)).astype(BF)
            part = dot(e, jnp.concatenate([jnp.where(head_mask[h], values[l], 0), ones], axis=1))
            total = part if total is None else total + part
        return (total[:, :cz] / jnp.where(any_head, total[:, cz:], 1.0)).astype(BF)

    for l in (2, 3):
        o_send[l - 2] = attended(l)
        to_partner(o_send.at[l - 2], o_recv.at[l - 2], 3 + l)
    for jj in range(2):
        o_own[jj] = attended(jj)
    for jj in range(2):
        whole_wait(o_recv.at[jj], recv_sem.at[5 + jj])
        att = o_own[jj].astype(F32) + o_recv[jj].astype(F32)
        gated = (att_gates[jj] * att).astype(BF)
        tokens[pl.ds(jj, res, stride=2), :] = middle[jj] + dot(gated, w_ao_ref[...])
    upd_send[...] = tokens[...].astype(BF).reshape(n, rows, 2, cz)
    exchange(lambda d: upd_send.at[d], upd_recv.at[:, me], 7)
    whole_wait(upd_recv, recv_sem.at[7])
    out_ref[...] = upd_recv[...].reshape(rows, res, cz)

    others = pl.ds(0, n - 1)
    passed = pl.ds(0, n - side)
    whole_wait(edge_recv.at[passed], send_sem.at[0])
    whole_wait(upd_send.at[passed], send_sem.at[1])
    whole_wait(prod_recv.at[others], send_sem.at[2])
    whole_wait(bias_recv.at[pl.ds(0, 2 * side - 1)], send_sem.at[3])
    whole_wait(att_peer, send_sem.at[4])
    whole_wait(o_recv.at[0], send_sem.at[5])
    whole_wait(o_recv.at[1], send_sem.at[6])
    whole_wait(upd_recv.at[:, others], send_sem.at[7])
    whole_wait(edge_mid.at[pl.ds(0, side - 1)], send_sem.at[8])
    whole_wait(pair_mid.at[pl.ds(0, side - 1)], send_sem.at[9])
    whole_wait(bias_recv.at[pl.ds(0, n - 2 * side)], send_sem.at[10])

def local(n, *args):
    args = [args[0], args[1].reshape(1, -1), *args[2:6], args[6].T, *args[7:]]
    rows, res, cz = args[0].shape
    side = math.isqrt(n // 2)
    pair_grid = (side, side, 2, rows, 2, cz)
    edge_grid = (side, side, 2, 2, 2, res)
    return pl.pallas_call(
        functools.partial(kernel, n),
        out_shape=pltpu.VMEM(args[0].shape, BF),
        in_specs=[pl.BlockSpec(memory_space=pl.ANY)] * len(args),
        out_specs=pl.BlockSpec(memory_space=pltpu.VMEM),
        scratch_shapes=[pltpu.VMEM(a.shape, a.dtype) for a in args]
        + [
            pltpu.VMEM(pair_grid, BF),
            pltpu.VMEM(pair_grid, BF),
            pltpu.VMEM(pair_grid, BF),
            pltpu.VMEM(edge_grid, BF),
            pltpu.VMEM(edge_grid, BF),
            pltpu.VMEM((n, 2, 2, res), BF),
            pltpu.VMEM((n, 2, res), BF),
            pltpu.VMEM((n, 2, res), BF),
            pltpu.VMEM((2 * res, cz), F32),
            pltpu.VMEM((2, res, cz), F32),
            pltpu.VMEM((2, res, cz), BF),
            pltpu.VMEM((2, res, cz), BF),
            pltpu.VMEM((2, 4, res), F32),
            pltpu.VMEM((n, 4, res), F32),
            pltpu.VMEM((8, res, res), F32),
            pltpu.VMEM((2, res, cz), BF),
            pltpu.VMEM((2, res, cz), BF),
            pltpu.VMEM((2, res, cz), BF),
            pltpu.VMEM((n, rows, 2, cz), BF),
            pltpu.VMEM((rows, n, 2, cz), BF),
            pltpu.SemaphoreType.DMA((len(args),)),
            pltpu.SemaphoreType.DMA((11,)),
            pltpu.SemaphoreType.DMA((8,)),
            pltpu.SemaphoreType.DMA((side,)),
            pltpu.SemaphoreType.DMA((side,)),
            pltpu.SemaphoreType.DMA((side,)),
            pltpu.SemaphoreType.REGULAR,
            pltpu.SemaphoreType.REGULAR,
        ],
        compiler_params=pltpu.CompilerParams(collective_id=0, has_side_effects=True),
        name="pair_update",
    )(*args)

def solution(mesh):
    split = P(("parts", "rows"), None, None)
    placed = (split, P("parts"), P(), P(), P(), P(), P(), P(), P())
    return jax.shard_map(
        functools.partial(local, mesh.shape["rows"]), mesh=mesh, in_specs=placed, out_specs=split, check_vma=False
    )
```

```python
import functools
import math
import random

import jax
import jax.numpy as jnp
from jax import lax
from jax.experimental import pallas as pl
from jax.experimental.pallas import tpu as pltpu
from jax.sharding import PartitionSpec as P

HEADS = 4
HEAD_DIM = 32
EPSILON = 1e-05
MASK_PENALTY = 1000000000.0
MESH = pl.DeviceIdType.MESH
BF = jnp.bfloat16
F32 = jnp.float32
NN = (((1,), (0,)), ((), ()))
NT = (((1,), (1,)), ((), ()))
TN = (((0,), (0,)), ((), ()))

def far_first(side):
    order = [(x, y, c) for x in range(side) for y in range(side) for c in range(2) if x + y + c]
    random.Random(1).shuffle(order)
    return sorted(order, key=lambda o: -(min(o[0], side - o[0]) + min(o[1], side - o[1])))

def dot(a, b, dims=NN):
    return lax.dot_general(a, b, dims, preferred_element_type=F32)

def sigmoid(x):
    return 0.5 * jnp.tanh(0.5 * x) + 0.5

def norm_lanes(x):
    center = jnp.mean(x, axis=1, keepdims=True)
    shifted = x - center
    spread = jnp.mean(shifted * shifted, axis=1, keepdims=True)
    return shifted * lax.rsqrt(spread + EPSILON)

def iota(shape, dim):
    return lax.broadcasted_iota(jnp.int32, shape, dim)

def spread_rows(rows, picked, parity):
    return (iota((rows, picked), 0) == 2 * iota((rows, picked), 1) + parity).astype(F32).astype(BF)

def whole_wait(ref, sem):
    pltpu.make_async_copy(ref, ref, sem).wait()

def kernel(
    n,
    pair_hbm, mask_hbm, w_in_hbm, w_tg_hbm, w_to_hbm, w_qkv_hbm, w_ab_hbm, w_ag_hbm, w_ao_hbm,
    out_ref,
    pair_ref, mask_ref, w_in_ref, w_tg_ref, w_to_ref, w_qkv_ref, w_ab_ref, w_ag_ref, w_ao_ref,
    pair_send, pair_mid, pair_recv, edge_send, edge_mid, edge_recv, prod_send, prod_recv,
    tokens, middle, att_own, att_peer, bias_send, bias_recv, scores, o_send, o_recv, o_own, upd_send, upd_recv,
    load_sem, send_sem, recv_sem, edge_sem, pair_sem, bias_sem, ready_sem, late_sem,
):
    loads = [
        pltpu.make_async_copy(hbm, ref, load_sem.at[i])
        for i, (hbm, ref) in enumerate(
            zip(
                (pair_hbm, mask_hbm, w_in_hbm, w_tg_hbm, w_to_hbm, w_qkv_hbm, w_ab_hbm, w_ag_hbm, w_ao_hbm),
                (pair_ref, mask_ref, w_in_ref, w_tg_ref, w_to_ref, w_qkv_ref, w_ab_ref, w_ag_ref, w_ao_ref),
            )
        )
    ]
    for load in loads:
        load.start()
    rows, res, cz = pair_ref.shape
    side = math.isqrt(n // 2)
    me = lax.axis_index("rows")
    core = lax.rem(me, 2)
    x = me // (2 * side)
    y = lax.rem(me // 2, side)
    partner = me + 1 - 2 * core
    lead = x + core * (y - x)
    far = sorted(range(1, side), key=lambda t: -min(t, side - t))
    near = sorted(range(1, side), key=lambda t: min(t, side - t))

    def chip(tx, ty):
        return lax.rem(x + tx, side) * side + lax.rem(y + ty, side)

    barrier = pltpu.get_barrier_semaphore()

    def greet(device):
        pl.semaphore_signal(barrier, inc=1, device_id={"rows": device}, device_id_type=MESH)

    first = me == 0
    beside_first = me == 1
    in_row = (y == 0) & (x > 0)
    in_column = (x == 0) & (y > 0)
    feeds_first = in_row & (core == 0)
    ends_at_first = (in_column & (core == 0)) | (in_row & (core == 1))

    @pl.when(me > 0)
    def _():
        for t in far:
            greet(2 * chip(t, 0))
            greet(2 * chip(0, t) + 1)
        greet(partner)

    def tell(sem, device):
        pl.semaphore_signal(sem, inc=1, device_id={"rows": device}, device_id_type=MESH)

    @pl.when(first)
    def _():
        pl.semaphore_wait(barrier, 2 * side - 1)
        tell(ready_sem, 1)
        pl.semaphore_wait(ready_sem, 1)
        for t in far:
            for c in range(2):
                tell(late_sem, 2 * side * t + c)
            tell(late_sem, 2 * t)

    def push(source, target, sent, received, device):
        copy = pltpu.make_async_remote_copy(
            src_ref=source, dst_ref=target, send_sem=send_sem.at[sent], recv_sem=received,
            device_id={"rows": device}, device_id_type=MESH,
        )
        copy.start()

    def first_leg(send_ref, mid_ref, sent, sems):
        @pl.when(core == 0)
        def _():
            for t in far:
                target = lax.rem(x + t, side)

                @pl.when((y > 0) | (target > 0))
                def _():
                    push(
                        send_ref.at[target], mid_ref.at[x], sent, sems.at[(side - t) % side],
                        2 * (target * side + y),
                    )

        @pl.when(core == 1)
        def _():
            for t in far:
                push(
                    send_ref.at[:, lax.rem(y + t, side)], mid_ref.at[y], sent, sems.at[(side - t) % side],
                    2 * chip(0, t) + 1,
                )

    def around_first(send_ref, recv_ref, sent, received):
        for t in far + [0]:
            for c in range(2):
                push(send_ref.at[0, t, c], recv_ref.at[x, 0, 0], sent, received, 2 * t + c)

    def own_leg(send_ref, mid_ref, sems):
        @pl.when(core == 0)
        def _():
            pltpu.make_async_copy(send_ref.at[x], mid_ref.at[x], sems.at[0]).start()

        @pl.when(core == 1)
        def _():
            pltpu.make_async_copy(send_ref.at[:, y], mid_ref.at[y], sems.at[0]).start()

    def second_leg(low, high, mid_ref, recv_ref, sent, sems, received, skip_first):
        span = pl.ds(low, high - low)
        for s in range(low, high):
            whole_wait(mid_ref.at[s], sems.at[lax.rem(s - lead + side, side)])
        for along in range(2):

            @pl.when(core == along)
            def _():
                target = recv_ref.at[x, span, 1] if along else recv_ref.at[span, y, 0]
                for t in far + [0]:
                    across = lax.rem((x if along else y) + t, side)
                    there = 2 * (chip(t, 0) if along else chip(0, t))
                    for c in (1 - along, along):
                        source = mid_ref.at[span, across, c]
                        if t and c == 0 and skip_first:

                            @pl.when(there > 0)
                            def _():
                                push(source, target, sent, received, there)
                        elif t or c != along:
                            push(source, target, sent, received, there + c)
                        else:
                            pltpu.make_async_copy(source, target, received).start()

    def second_leg_late(low, high, mid_ref, recv_ref, sent, received):
        span = pl.ds(low, high - low)
        for along in range(2):

            @pl.when(core == along)
            def _():
                target = recv_ref.at[x, span, 1] if along else recv_ref.at[span, y, 0]
                push(mid_ref.at[span, 0, 0], target, sent, received, 0)

    def exchange(source, target, k):
        for tx, ty, tc in far_first(side):
            d = 2 * chip(tx, ty) + core + tc - 2 * core * tc
            push(source(d), target, k, recv_sem.at[k], d)
        pltpu.make_async_copy(source(me), target, recv_sem.at[k]).start()

    def to_partner(source, target, k):
        push(source, target, k, recv_sem.at[k], partner)

    for load in loads:
        load.wait()

    key_mask = mask_ref[...].astype(F32)
    lane = iota((1, res), 1)
    row_mask = [
        jnp.sum(jnp.where(lane == me * rows + r, key_mask, 0.0), axis=1, keepdims=True) for r in range(rows)
    ]
    spreads = [spread_rows(2 * cz, cz, r) for r in range(2)]
    for r in range(rows):
        pair_send[:, :, :, r] = pair_ref[r].reshape(side, side, 2, 2, cz)
    normed = jnp.concatenate(
        [norm_lanes(pair_ref[r].astype(F32)).astype(BF) for r in range(rows)], axis=1
    )

    def projected(g):
        w = w_in_ref[:, g * cz : (g + 1) * cz]
        spread_w = jnp.concatenate([dot(s, w, NT).astype(BF) for s in spreads], axis=1)
        return dot(spread_w, normed, NT)

    parity = iota((2 * cz, res), 0) % 2
    pair_mask = jnp.where(parity == 0, row_mask[0], row_mask[1]) * key_mask
    for a in range(2):
        edge = (sigmoid(projected(2 * a)) * projected(2 * a + 1) * pair_mask).astype(BF)
        edge_send[:, :, :, a] = edge.reshape(side, side, 2, 2, res)

    @pl.when(me > 0)
    def _():
        absent = feeds_first | ((x == 0) & (core == 1))
        pl.semaphore_wait(barrier, 2 * side - 1 - absent.astype(jnp.int32))

        @pl.when(me > 1)
        def _():
            tell(ready_sem, partner)

    edge_legs = (edge_mid, edge_recv, 0, edge_sem, recv_sem.at[0])
    pair_legs = (pair_mid, pair_recv, 1, pair_sem, recv_sem.at[1])
    spans = ((side // 2, side), (1, side // 2), (0, 1))
    first_leg(edge_send, edge_mid, 8, edge_sem)
    own_leg(edge_send, edge_mid, edge_sem)
    first_leg(pair_send, pair_mid, 9, pair_sem)
    own_leg(pair_send, pair_mid, pair_sem)
    @pl.when(me > 0)
    def _():
        pl.semaphore_wait(ready_sem, 1)

        @pl.when(beside_first)
        def _():
            tell(ready_sem, 0)

        for low, high in spans[:2]:
            second_leg(low, high, *edge_legs, True)

        @pl.when(feeds_first)
        def _():
            pl.semaphore_wait(late_sem, 1)
            around_first(edge_send, edge_recv, 8, recv_sem.at[0])

    second_leg(*spans[2], *edge_legs, True)

    @pl.when(feeds_first)
    def _():
        around_first(pair_send, pair_recv, 9, recv_sem.at[1])

    @pl.when(ends_at_first)
    def _():
        pl.semaphore_wait(late_sem, 1)
        for low, high in spans:
            second_leg_late(low, high, edge_mid, edge_recv, 0, recv_sem.at[0])

    @pl.when(me > 0)
    def _():
        second_leg(0, side, *pair_legs, False)

    @pl.when(first)
    def _():
        second_leg(0, 1, *pair_legs, False)

    whole_wait(edge_recv, recv_sem.at[0])
    left = edge_recv[:, :, :, 0].reshape(res, res)
    right = edge_recv[:, :, :, 1].reshape(res, res)
    prod_send[...] = dot(right, left, NT).astype(BF).reshape(n, 2, res)
    exchange(lambda d: prod_send.at[d], prod_recv.at[me], 2)

    whole_wait(pair_recv, recv_sem.at[1])
    tokens[...] = pair_recv[...].reshape(2 * res, cz).astype(F32)
    columns = [tokens[pl.ds(jj, res, stride=2), :] for jj in range(2)]
    gates = [sigmoid(dot(norm_lanes(x).astype(BF), w_tg_ref[...])) for x in columns]
    w_to = w_to_ref[...]
    spread_out = jnp.concatenate([dot(s, w_to).astype(BF) for s in spreads], axis=1)
    e_row = iota((8, HEADS), 0)
    e_col = iota((8, HEADS), 1)
    w_bias = jnp.concatenate(
        [
            dot(((e_row // 2 == e_col) & (e_row % 2 == jj)).astype(F32).astype(BF), w_ab_ref[...]).astype(BF)
            for jj in range(2)
        ],
        axis=1,
    )

    whole_wait(prod_recv, recv_sem.at[2])
    product = prod_recv[...].reshape(2 * cz, res).astype(F32)
    sub = iota((8, res), 0) % 2

    def column_mean(x):
        total = jnp.sum(x.reshape(2 * cz // 8, 8, res), axis=0)
        even = jnp.sum(jnp.where(sub == 0, total, 0.0), axis=0, keepdims=True)
        odd = jnp.sum(jnp.where(sub == 0, 0.0, total), axis=0, keepdims=True)
        return jnp.where(sub == 0, even, odd) * (1.0 / cz)

    tall = product.reshape(2 * cz // 8, 8, res)
    tall = tall - column_mean(product)[None]
    spread = column_mean((tall * tall).reshape(2 * cz, res))
    tri = (tall * lax.rsqrt(spread + EPSILON)[None]).reshape(2 * cz, res).astype(BF)
    update = dot(tri, spread_out, TN)
    for jj in range(2):
        mid = (columns[jj] + gates[jj] * update[:, jj * cz : (jj + 1) * cz]).astype(BF).astype(F32)
        middle[jj] = mid
        att_own[jj] = norm_lanes(mid).astype(BF)
    to_partner(att_own, att_peer, 4)
    both = jnp.concatenate([att_own[0], att_own[1]], axis=1)
    bias_send[...] = dot(w_bias, both, NT).reshape(2, 4, res)
    for t in far:
        push(bias_send.at[0], bias_recv.at[me], 3, bias_sem.at[(side - t) % side], 2 * chip(t, 0))
        push(bias_send.at[1], bias_recv.at[me], 3, bias_sem.at[(side - t) % side], 2 * chip(0, t) + 1)
    push(bias_send.at[1 - core], bias_recv.at[me], 3, bias_sem.at[0], partner)
    pltpu.make_async_copy(bias_send.at[core], bias_recv.at[me], bias_sem.at[0]).start()

    def pass_on(u):
        s = lax.rem(lead + u, side)
        block = bias_recv.at[pl.ds(2 * ((s + core * (x - s)) * side + y + core * (s - y)), 2)]
        whole_wait(block, bias_sem.at[u])
        for t in far:
            push(block, block, 10, recv_sem.at[3], 2 * chip(core * t, (1 - core) * t) + core)

    penalty = (key_mask - 1.0) * MASK_PENALTY
    lane_head = iota((1, cz), 1) // HEAD_DIM
    head_mask = [lane_head == 2 * core + h for h in range(2)]
    values = []

    def score(rows_in):
        qkv = dot(rows_in, w_qkv_ref[...]).astype(BF)
        for h in range(2):
            key = jnp.where(head_mask[h], qkv[:, cz : 2 * cz], 0)
            scores[2 * len(values) + h] = dot(qkv[:, :cz], key, NT) * (HEAD_DIM ** -0.5) + penalty
        values.append(qkv[:, 2 * cz :])

    score(att_own[0])
    pass_on(0)
    score(att_own[1])
    whole_wait(att_peer, recv_sem.at[4])
    pass_on(near[0])
    pass_on(near[1])
    score(att_peer[0])
    pass_on(near[2])
    pass_on(near[3])
    score(att_peer[1])
    for u in near[4:]:
        pass_on(u)
    att_gates = [sigmoid(dot(att_own[jj], w_ag_ref[...])) for jj in range(2)]

    whole_wait(bias_recv.at[pl.ds(0, n - 2 * side)], recv_sem.at[3])
    any_head = head_mask[0] | head_mask[1]

    def attended(l):
        total = None
        for h in range(2):
            s = scores[2 * l + h] + bias_recv[:, 2 * h : 2 * h + 2].reshape(res, res)
            e = jnp.exp(s - jnp.max(s, axis=1, keepdims=True)).astype(BF)
            ones = jnp.broadcast_to(jnp.where(head_mask[h], 1.0, 0.0), (res, cz)).astype(BF)
            part = dot(e, jnp.concatenate([jnp.where(head_mask[h], values[l], 0), ones], axis=1))
            total = part if total is None else total + part
        return (total[:, :cz] / jnp.where(any_head, total[:, cz:], 1.0)).astype(BF)

    for l in (2, 3):
        o_send[l - 2] = attended(l)
        to_partner(o_send.at[l - 2], o_recv.at[l - 2], 3 + l)
    for jj in range(2):
        o_own[jj] = attended(jj)
    for jj in range(2):
        whole_wait(o_recv.at[jj], recv_sem.at[5 + jj])
        att = o_own[jj].astype(F32) + o_recv[jj].astype(F32)
        gated = (att_gates[jj] * att).astype(BF)
        tokens[pl.ds(jj, res, stride=2), :] = middle[jj] + dot(gated, w_ao_ref[...])
    upd_send[...] = tokens[...].astype(BF).reshape(n, rows, 2, cz)
    exchange(lambda d: upd_send.at[d], upd_recv.at[:, me], 7)
    whole_wait(upd_recv, recv_sem.at[7])
    out_ref[...] = upd_recv[...].reshape(rows, res, cz)

    others = pl.ds(0, n - 1)
    passed = pl.ds(0, n - side)

    @pl.when(me > 0)
    def _():
        whole_wait(bias_recv.at[pl.ds(0, (n - side) // 2)], send_sem.at[0])
        whole_wait(upd_send.at[passed], send_sem.at[1])

    @pl.when(first)
    def _():
        whole_wait(upd_send.at[pl.ds(0, 4 * side - 2)], send_sem.at[0])
        whole_wait(upd_send.at[pl.ds(0, 2 * side - 1)], send_sem.at[1])

    whole_wait(prod_recv.at[others], send_sem.at[2])
    whole_wait(bias_recv.at[pl.ds(0, 2 * side - 1)], send_sem.at[3])
    whole_wait(att_peer, send_sem.at[4])
    whole_wait(o_recv.at[0], send_sem.at[5])
    whole_wait(o_recv.at[1], send_sem.at[6])
    whole_wait(upd_recv.at[:, others], send_sem.at[7])
    whole_wait(edge_mid.at[pl.ds(0, side - 1)], send_sem.at[8])
    whole_wait(pair_mid.at[pl.ds(0, side - 1)], send_sem.at[9])
    whole_wait(bias_recv.at[pl.ds(0, n - 2 * side)], send_sem.at[10])

def local(n, *args):
    args = [args[0], args[1].reshape(1, -1), *args[2:6], args[6].T, *args[7:]]
    rows, res, cz = args[0].shape
    side = math.isqrt(n // 2)
    pair_grid = (side, side, 2, rows, 2, cz)
    edge_grid = (side, side, 2, 2, 2, res)
    return pl.pallas_call(
        functools.partial(kernel, n),
        out_shape=pltpu.VMEM(args[0].shape, BF),
        in_specs=[pl.BlockSpec(memory_space=pl.ANY)] * len(args),
        out_specs=pl.BlockSpec(memory_space=pltpu.VMEM),
        scratch_shapes=[pltpu.VMEM(a.shape, a.dtype) for a in args]
        + [
            pltpu.VMEM(pair_grid, BF),
            pltpu.VMEM(pair_grid, BF),
            pltpu.VMEM(pair_grid, BF),
            pltpu.VMEM(edge_grid, BF),
            pltpu.VMEM(edge_grid, BF),
            pltpu.VMEM(edge_grid, BF),
            pltpu.VMEM((n, 2, res), BF),
            pltpu.VMEM((n, 2, res), BF),
            pltpu.VMEM((2 * res, cz), F32),
            pltpu.VMEM((2, res, cz), F32),
            pltpu.VMEM((2, res, cz), BF),
            pltpu.VMEM((2, res, cz), BF),
            pltpu.VMEM((2, 4, res), F32),
            pltpu.VMEM((n, 4, res), F32),
            pltpu.VMEM((8, res, res), F32),
            pltpu.VMEM((2, res, cz), BF),
            pltpu.VMEM((2, res, cz), BF),
            pltpu.VMEM((2, res, cz), BF),
            pltpu.VMEM((n, rows, 2, cz), BF),
            pltpu.VMEM((rows, n, 2, cz), BF),
            pltpu.SemaphoreType.DMA((len(args),)),
            pltpu.SemaphoreType.DMA((11,)),
            pltpu.SemaphoreType.DMA((8,)),
            pltpu.SemaphoreType.DMA((side,)),
            pltpu.SemaphoreType.DMA((side,)),
            pltpu.SemaphoreType.DMA((side,)),
            pltpu.SemaphoreType.REGULAR,
            pltpu.SemaphoreType.REGULAR,
        ],
        compiler_params=pltpu.CompilerParams(collective_id=0, has_side_effects=True),
        name="pair_update",
    )(*args)

def solution(mesh):
    split = P(("parts", "rows"), None, None)
    placed = (split, P("parts"), P(), P(), P(), P(), P(), P(), P())
    return jax.shard_map(
        functools.partial(local, mesh.shape["rows"]), mesh=mesh, in_specs=placed, out_specs=split, check_vma=False
    )
```

```python
import functools
import math
import random

import jax
import jax.numpy as jnp
from jax import lax
from jax.experimental import pallas as pl
from jax.experimental.pallas import tpu as pltpu
from jax.sharding import PartitionSpec as P

HEADS = 4
HEAD_DIM = 32
EPSILON = 1e-05
MASK_PENALTY = 1000000000.0
MESH = pl.DeviceIdType.MESH
BF = jnp.bfloat16
F32 = jnp.float32
NN = (((1,), (0,)), ((), ()))
NT = (((1,), (1,)), ((), ()))
TN = (((0,), (0,)), ((), ()))

def far_first(side):
    order = [(x, y, c) for x in range(side) for y in range(side) for c in range(2) if x + y + c]
    random.Random(1).shuffle(order)
    return sorted(order, key=lambda o: -(min(o[0], side - o[0]) + min(o[1], side - o[1])))

def dot(a, b, dims=NN):
    return lax.dot_general(a, b, dims, preferred_element_type=F32)

def sigmoid(x):
    return 0.5 * jnp.tanh(0.5 * x) + 0.5

def norm_lanes(x):
    center = jnp.mean(x, axis=1, keepdims=True)
    shifted = x - center
    spread = jnp.mean(shifted * shifted, axis=1, keepdims=True)
    return shifted * lax.rsqrt(spread + EPSILON)

def iota(shape, dim):
    return lax.broadcasted_iota(jnp.int32, shape, dim)

def spread_rows(rows, picked, parity):
    return (iota((rows, picked), 0) == 2 * iota((rows, picked), 1) + parity).astype(F32).astype(BF)

def whole_wait(ref, sem):
    pltpu.make_async_copy(ref, ref, sem).wait()

def kernel(
    n,
    pair_hbm, mask_hbm, w_in_hbm, w_tg_hbm, w_to_hbm, w_qkv_hbm, w_ab_hbm, w_ag_hbm, w_ao_hbm,
    out_ref,
    pair_ref, mask_ref, w_in_ref, w_tg_ref, w_to_ref, w_qkv_ref, w_ab_ref, w_ag_ref, w_ao_ref,
    pair_send, pair_mid, pair_recv, edge_send, edge_mid, edge_recv, prod_send, prod_recv,
    tokens, middle, att_own, att_peer, bias_send, bias_recv, scores, o_send, o_recv, o_own, upd_send, upd_recv,
    load_sem, send_sem, recv_sem, edge_sem, pair_sem, bias_sem, ready_sem, late_sem, row_sem,
):
    loads = [
        pltpu.make_async_copy(hbm, ref, load_sem.at[i])
        for i, (hbm, ref) in enumerate(
            zip(
                (pair_hbm, mask_hbm, w_in_hbm, w_tg_hbm, w_to_hbm, w_qkv_hbm, w_ab_hbm, w_ag_hbm, w_ao_hbm),
                (pair_ref, mask_ref, w_in_ref, w_tg_ref, w_to_ref, w_qkv_ref, w_ab_ref, w_ag_ref, w_ao_ref),
            )
        )
    ]
    for load in loads:
        load.start()
    rows, res, cz = pair_ref.shape
    side = math.isqrt(n // 2)
    me = lax.axis_index("rows")
    core = lax.rem(me, 2)
    x = me // (2 * side)
    y = lax.rem(me // 2, side)
    partner = me + 1 - 2 * core
    lead = x + core * (y - x)
    far = sorted(range(1, side), key=lambda t: -min(t, side - t))
    near = sorted(range(1, side), key=lambda t: min(t, side - t))

    def chip(tx, ty):
        return lax.rem(x + tx, side) * side + lax.rem(y + ty, side)

    barrier = pltpu.get_barrier_semaphore()

    def greet(device):
        pl.semaphore_signal(barrier, inc=1, device_id={"rows": device}, device_id_type=MESH)

    first = me == 0
    in_row = (y == 0) & (x > 0)
    in_column = (x == 0) & (y > 0)
    feeds_first = in_row & (core == 0)
    ends_at_first = (in_column & (core == 0)) | (in_row & (core == 1))

    @pl.when(me > 0)
    def _():
        for t in far:

            @pl.when((y > 0) | (core == 1) | (lax.rem(x + t, side) > 0))
            def _():
                greet(2 * chip(t, 0))

            greet(2 * chip(0, t) + 1)
        greet(partner)

    def tell(sem, device):
        pl.semaphore_signal(sem, inc=1, device_id={"rows": device}, device_id_type=MESH)

    def push(source, target, sent, received, device):
        copy = pltpu.make_async_remote_copy(
            src_ref=source, dst_ref=target, send_sem=send_sem.at[sent], recv_sem=received,
            device_id={"rows": device}, device_id_type=MESH,
        )
        copy.start()

    def first_leg(send_ref, mid_ref, sent, sems):
        @pl.when(core == 0)
        def _():
            for t in far:
                target = lax.rem(x + t, side)

                @pl.when((y > 0) | (target > 0))
                def _():
                    push(
                        send_ref.at[target], mid_ref.at[x], sent, sems.at[(side - t) % side],
                        2 * (target * side + y),
                    )

        @pl.when(core == 1)
        def _():
            for t in far:
                push(
                    send_ref.at[:, lax.rem(y + t, side)], mid_ref.at[y], sent, sems.at[(side - t) % side],
                    2 * chip(0, t) + 1,
                )

    def around_first(send_ref, recv_ref, sent, received):
        for t in far + [0]:
            for c in range(2):
                if t or c:
                    push(send_ref.at[0, t, c], recv_ref.at[x, 0, 0], sent, received, 2 * t + c)

    def from_first(send_ref, recv_ref, sents, received):
        for tx, ty, tc in far_first(side):
            push(send_ref.at[tx, ty, tc], recv_ref.at[0, 0, 0], sents[tc], received, 2 * (tx * side + ty) + tc)
        pltpu.make_async_copy(send_ref.at[0, 0, 0], recv_ref.at[0, 0, 0], received).start()

    def own_leg(send_ref, mid_ref, sems):
        @pl.when(core == 0)
        def _():
            pltpu.make_async_copy(send_ref.at[x], mid_ref.at[x], sems.at[0]).start()

        @pl.when(core == 1)
        def _():
            pltpu.make_async_copy(send_ref.at[:, y], mid_ref.at[y], sems.at[0]).start()

    def second_leg(low, high, mid_ref, recv_ref, sent, sems, received, skip_first):
        span = pl.ds(low, high - low)
        for s in range(low, high):
            whole_wait(mid_ref.at[s], sems.at[lax.rem(s - lead + side, side)])
        for along in range(2):

            @pl.when(core == along)
            def _():
                target = recv_ref.at[x, span, 1] if along else recv_ref.at[span, y, 0]
                for t in far + [0]:
                    across = lax.rem((x if along else y) + t, side)
                    there = 2 * (chip(t, 0) if along else chip(0, t))
                    for c in (1 - along, along):
                        source = mid_ref.at[span, across, c]
                        if t and c == 0 and skip_first:

                            @pl.when(there > 0)
                            def _():
                                push(source, target, sent, received, there)
                        elif t or c != along:
                            push(source, target, sent, received, there + c)
                        else:
                            pltpu.make_async_copy(source, target, received).start()

    def second_leg_late(low, high, mid_ref, recv_ref, sent, received):
        span = pl.ds(low, high - low)
        for along in range(2):

            @pl.when(core == along)
            def _():
                target = recv_ref.at[x, span, 1] if along else recv_ref.at[span, y, 0]
                push(mid_ref.at[span, 0, 0], target, sent, received, 0)

    def exchange(source, target, k):
        for tx, ty, tc in far_first(side):
            d = 2 * chip(tx, ty) + core + tc - 2 * core * tc
            push(source(d), target, k, recv_sem.at[k], d)
        pltpu.make_async_copy(source(me), target, recv_sem.at[k]).start()

    def to_partner(source, target, k):
        push(source, target, k, recv_sem.at[k], partner)

    for load in loads[:3]:
        load.wait()

    key_mask = mask_ref[...].astype(F32)
    lane = iota((1, res), 1)
    row_mask = [
        jnp.sum(jnp.where(lane == me * rows + r, key_mask, 0.0), axis=1, keepdims=True) for r in range(rows)
    ]
    spreads = [spread_rows(2 * cz, cz, r) for r in range(2)]
    normed = jnp.concatenate(
        [norm_lanes(pair_ref[r].astype(F32)).astype(BF) for r in range(rows)], axis=1
    )

    def projected(g):
        w = w_in_ref[:, g * cz : (g + 1) * cz]
        spread_w = jnp.concatenate([dot(s, w, NT).astype(BF) for s in spreads], axis=1)
        return dot(spread_w, normed, NT)

    parity = iota((2 * cz, res), 0) % 2
    pair_mask = jnp.where(parity == 0, row_mask[0], row_mask[1]) * key_mask
    for a in range(2):
        edge = (sigmoid(projected(2 * a)) * projected(2 * a + 1) * pair_mask).astype(BF)
        edge_send[:, :, :, a] = edge.reshape(side, side, 2, 2, res)

    @pl.when(me > 0)
    def _():
        absent = feeds_first | ((x == 0) & (core == 1))
        pl.semaphore_wait(barrier, 2 * side - 1 - absent.astype(jnp.int32))

        @pl.when(me > 1)
        def _():
            tell(ready_sem, partner)

    edge_legs = (edge_mid, edge_recv, 0, edge_sem, recv_sem.at[0])
    pair_legs = (pair_mid, pair_recv, 1, pair_sem, recv_sem.at[1])
    spans = ((side // 2, side), (1, side // 2), (0, 1))

    @pl.when(first)
    def _():
        pl.semaphore_wait(barrier, 2 * side - 1)
        tell(ready_sem, 1)
        for t in far:
            for c in range(2):
                tell(late_sem, 2 * side * t + c)
            tell(late_sem, 2 * t)
        from_first(edge_send, edge_recv, (0, 8), recv_sem.at[0])

    @pl.when(me > 0)
    def _():
        first_leg(edge_send, edge_mid, 8, edge_sem)
        own_leg(edge_send, edge_mid, edge_sem)

    for r in range(rows):
        pair_send[:, :, :, r] = pair_ref[r].reshape(side, side, 2, 2, cz)
    for load in loads[3:]:
        load.wait()

    @pl.when(first)
    def _():
        from_first(pair_send, pair_recv, (1, 1), recv_sem.at[1])

    @pl.when(me > 0)
    def _():
        first_leg(pair_send, pair_mid, 9, pair_sem)
        own_leg(pair_send, pair_mid, pair_sem)
        pl.semaphore_wait(ready_sem, 1)

        @pl.when((core == 0) & (x > 0) & (y > 0))
        def _():
            tell(row_sem, 2 * side * x)

        @pl.when(feeds_first)
        def _():
            pl.semaphore_wait(row_sem, side - 1)
            greet(0)

        for low, high in spans[:2]:
            second_leg(low, high, *edge_legs, True)

        @pl.when(feeds_first)
        def _():
            around_first(edge_send, edge_recv, 8, recv_sem.at[0])
            around_first(pair_send, pair_recv, 9, recv_sem.at[1])
            pl.semaphore_wait(late_sem, 1)
            push(edge_send.at[0, 0, 0], edge_recv.at[x, 0, 0], 8, recv_sem.at[0], 0)
            push(pair_send.at[0, 0, 0], pair_recv.at[x, 0, 0], 9, recv_sem.at[1], 0)
            second_leg(1, side, *pair_legs, False)

        @pl.when(jnp.logical_not(feeds_first))
        def _():
            second_leg(*spans[2], *edge_legs, True)

            @pl.when(ends_at_first)
            def _():
                pl.semaphore_wait(late_sem, 1)
                for low, high in spans:
                    second_leg_late(low, high, edge_mid, edge_recv, 0, recv_sem.at[0])

            second_leg(0, side, *pair_legs, False)

    whole_wait(edge_recv, recv_sem.at[0])
    left = edge_recv[:, :, :, 0].reshape(res, res)
    right = edge_recv[:, :, :, 1].reshape(res, res)
    prod_send[...] = dot(right, left, NT).astype(BF).reshape(n, 2, res)
    exchange(lambda d: prod_send.at[d], prod_recv.at[me], 2)

    whole_wait(pair_recv, recv_sem.at[1])
    tokens[...] = pair_recv[...].reshape(2 * res, cz).astype(F32)
    columns = [tokens[pl.ds(jj, res, stride=2), :] for jj in range(2)]
    gates = [sigmoid(dot(norm_lanes(x).astype(BF), w_tg_ref[...])) for x in columns]
    w_to = w_to_ref[...]
    spread_out = jnp.concatenate([dot(s, w_to).astype(BF) for s in spreads], axis=1)
    e_row = iota((8, HEADS), 0)
    e_col = iota((8, HEADS), 1)
    w_bias = jnp.concatenate(
        [
            dot(((e_row // 2 == e_col) & (e_row % 2 == jj)).astype(F32).astype(BF), w_ab_ref[...]).astype(BF)
            for jj in range(2)
        ],
        axis=1,
    )

    whole_wait(prod_recv, recv_sem.at[2])
    product = prod_recv[...].reshape(2 * cz, res).astype(F32)
    sub = iota((8, res), 0) % 2

    def column_mean(x):
        total = jnp.sum(x.reshape(2 * cz // 8, 8, res), axis=0)
        even = jnp.sum(jnp.where(sub == 0, total, 0.0), axis=0, keepdims=True)
        odd = jnp.sum(jnp.where(sub == 0, 0.0, total), axis=0, keepdims=True)
        return jnp.where(sub == 0, even, odd) * (1.0 / cz)

    tall = product.reshape(2 * cz // 8, 8, res)
    tall = tall - column_mean(product)[None]
    spread = column_mean((tall * tall).reshape(2 * cz, res))
    tri = (tall * lax.rsqrt(spread + EPSILON)[None]).reshape(2 * cz, res).astype(BF)
    update = dot(tri, spread_out, TN)
    for jj in range(2):
        mid = (columns[jj] + gates[jj] * update[:, jj * cz : (jj + 1) * cz]).astype(BF).astype(F32)
        middle[jj] = mid
        att_own[jj] = norm_lanes(mid).astype(BF)
    to_partner(att_own, att_peer, 4)
    both = jnp.concatenate([att_own[0], att_own[1]], axis=1)
    bias_send[...] = dot(w_bias, both, NT).reshape(2, 4, res)
    for t in far:
        push(bias_send.at[0], bias_recv.at[me], 3, bias_sem.at[(side - t) % side], 2 * chip(t, 0))
        push(bias_send.at[1], bias_recv.at[me], 3, bias_sem.at[(side - t) % side], 2 * chip(0, t) + 1)
    push(bias_send.at[1 - core], bias_recv.at[me], 3, bias_sem.at[0], partner)
    pltpu.make_async_copy(bias_send.at[core], bias_recv.at[me], bias_sem.at[0]).start()

    def pass_on(u):
        s = lax.rem(lead + u, side)
        block = bias_recv.at[pl.ds(2 * ((s + core * (x - s)) * side + y + core * (s - y)), 2)]
        whole_wait(block, bias_sem.at[u])
        for t in far:
            push(block, block, 10, recv_sem.at[3], 2 * chip(core * t, (1 - core) * t) + core)

    penalty = (key_mask - 1.0) * MASK_PENALTY
    lane_head = iota((1, cz), 1) // HEAD_DIM
    head_mask = [lane_head == 2 * core + h for h in range(2)]
    values = []

    def score(rows_in):
        qkv = dot(rows_in, w_qkv_ref[...]).astype(BF)
        for h in range(2):
            key = jnp.where(head_mask[h], qkv[:, cz : 2 * cz], 0)
            scores[2 * len(values) + h] = dot(qkv[:, :cz], key, NT) * (HEAD_DIM ** -0.5) + penalty
        values.append(qkv[:, 2 * cz :])

    score(att_own[0])
    pass_on(0)
    score(att_own[1])
    whole_wait(att_peer, recv_sem.at[4])
    pass_on(near[0])
    pass_on(near[1])
    score(att_peer[0])
    pass_on(near[2])
    pass_on(near[3])
    score(att_peer[1])
    for u in near[4:]:
        pass_on(u)
    att_gates = [sigmoid(dot(att_own[jj], w_ag_ref[...])) for jj in range(2)]

    whole_wait(bias_recv.at[pl.ds(0, n - 2 * side)], recv_sem.at[3])
    any_head = head_mask[0] | head_mask[1]

    def attended(l):
        total = None
        for h in range(2):
            s = scores[2 * l + h] + bias_recv[:, 2 * h : 2 * h + 2].reshape(res, res)
            e = jnp.exp(s - jnp.max(s, axis=1, keepdims=True)).astype(BF)
            ones = jnp.broadcast_to(jnp.where(head_mask[h], 1.0, 0.0), (res, cz)).astype(BF)
            part = dot(e, jnp.concatenate([jnp.where(head_mask[h], values[l], 0), ones], axis=1))
            total = part if total is None else total + part
        return (total[:, :cz] / jnp.where(any_head, total[:, cz:], 1.0)).astype(BF)

    for l in (2, 3):
        o_send[l - 2] = attended(l)
        to_partner(o_send.at[l - 2], o_recv.at[l - 2], 3 + l)
    for jj in range(2):
        o_own[jj] = attended(jj)
    for jj in range(2):
        middle[jj] = middle[jj] + dot((att_gates[jj] * o_own[jj].astype(F32)).astype(BF), w_ao_ref[...])
    for jj in range(2):
        whole_wait(o_recv.at[jj], recv_sem.at[5 + jj])
        gated = (att_gates[jj] * o_recv[jj].astype(F32)).astype(BF)
        tokens[pl.ds(jj, res, stride=2), :] = middle[jj] + dot(gated, w_ao_ref[...])
    upd_send[...] = tokens[...].astype(BF).reshape(n, rows, 2, cz)
    exchange(lambda d: upd_send.at[d], upd_recv.at[:, me], 7)
    whole_wait(upd_recv, recv_sem.at[7])
    out_ref[...] = upd_recv[...].reshape(rows, res, cz)

    others = pl.ds(0, n - 1)
    passed = pl.ds(0, n - side)

    half = pl.ds(0, res // 2)
    ahead = (side - 1) * (2 * side - 1)

    @pl.when(feeds_first)
    def _():
        whole_wait(bias_recv.at[pl.ds(0, ahead), :, half], send_sem.at[0])
        whole_wait(upd_send.at[pl.ds(0, ahead)], send_sem.at[1])

    @pl.when((me > 0) & jnp.logical_not(feeds_first))
    def _():
        whole_wait(bias_recv.at[passed, :, half], send_sem.at[0])
        whole_wait(upd_send.at[passed], send_sem.at[1])

    @pl.when(me > 0)
    def _():
        whole_wait(edge_mid.at[pl.ds(0, side - 1)], send_sem.at[8])
        whole_wait(pair_mid.at[pl.ds(0, side - 1)], send_sem.at[9])

    @pl.when(first)
    def _():
        whole_wait(prod_send.at[pl.ds(0, n - 2)], send_sem.at[0])
        whole_wait(prod_send, send_sem.at[8])
        whole_wait(upd_send.at[others], send_sem.at[1])

    whole_wait(prod_recv.at[others], send_sem.at[2])
    whole_wait(bias_recv.at[pl.ds(0, 2 * side - 1)], send_sem.at[3])
    whole_wait(att_peer, send_sem.at[4])
    whole_wait(o_recv.at[0], send_sem.at[5])
    whole_wait(o_recv.at[1], send_sem.at[6])
    whole_wait(upd_recv.at[:, others], send_sem.at[7])
    whole_wait(bias_recv.at[pl.ds(0, n - 2 * side)], send_sem.at[10])

def local(n, *args):
    args = [args[0], args[1].reshape(1, -1), *args[2:6], args[6].T, *args[7:]]
    rows, res, cz = args[0].shape
    side = math.isqrt(n // 2)
    pair_grid = (side, side, 2, rows, 2, cz)
    edge_grid = (side, side, 2, 2, 2, res)
    return pl.pallas_call(
        functools.partial(kernel, n),
        out_shape=pltpu.VMEM(args[0].shape, BF),
        in_specs=[pl.BlockSpec(memory_space=pl.ANY)] * len(args),
        out_specs=pl.BlockSpec(memory_space=pltpu.VMEM),
        scratch_shapes=[pltpu.VMEM(a.shape, a.dtype) for a in args]
        + [
            pltpu.VMEM(pair_grid, BF),
            pltpu.VMEM(pair_grid, BF),
            pltpu.VMEM(pair_grid, BF),
            pltpu.VMEM(edge_grid, BF),
            pltpu.VMEM(edge_grid, BF),
            pltpu.VMEM(edge_grid, BF),
            pltpu.VMEM((n, 2, res), BF),
            pltpu.VMEM((n, 2, res), BF),
            pltpu.VMEM((2 * res, cz), F32),
            pltpu.VMEM((2, res, cz), F32),
            pltpu.VMEM((2, res, cz), BF),
            pltpu.VMEM((2, res, cz), BF),
            pltpu.VMEM((2, 4, res), F32),
            pltpu.VMEM((n, 4, res), F32),
            pltpu.VMEM((8, res, res), F32),
            pltpu.VMEM((2, res, cz), BF),
            pltpu.VMEM((2, res, cz), BF),
            pltpu.VMEM((2, res, cz), BF),
            pltpu.VMEM((n, rows, 2, cz), BF),
            pltpu.VMEM((rows, n, 2, cz), BF),
            pltpu.SemaphoreType.DMA((len(args),)),
            pltpu.SemaphoreType.DMA((11,)),
            pltpu.SemaphoreType.DMA((8,)),
            pltpu.SemaphoreType.DMA((side,)),
            pltpu.SemaphoreType.DMA((side,)),
            pltpu.SemaphoreType.DMA((side,)),
            pltpu.SemaphoreType.REGULAR,
            pltpu.SemaphoreType.REGULAR,
            pltpu.SemaphoreType.REGULAR,
        ],
        compiler_params=pltpu.CompilerParams(collective_id=0, has_side_effects=True),
        name="pair_update",
    )(*args)

def solution(mesh):
    split = P(("parts", "rows"), None, None)
    placed = (split, P("parts"), P(), P(), P(), P(), P(), P(), P())
    return jax.shard_map(
        functools.partial(local, mesh.shape["rows"]), mesh=mesh, in_specs=placed, out_specs=split, check_vma=False
    )
```

```python
import functools
import math
import random

import jax
import jax.numpy as jnp
from jax import lax
from jax.experimental import pallas as pl
from jax.experimental.pallas import tpu as pltpu
from jax.sharding import PartitionSpec as P

HEADS = 4
HEAD_DIM = 32
EPSILON = 1e-05
MASK_PENALTY = 1000000000.0
MESH = pl.DeviceIdType.MESH
BF = jnp.bfloat16
F32 = jnp.float32
NN = (((1,), (0,)), ((), ()))
NT = (((1,), (1,)), ((), ()))
TN = (((0,), (0,)), ((), ()))

def far_first(side):
    order = [(x, y, c) for x in range(side) for y in range(side) for c in range(2) if x + y + c]
    random.Random(1).shuffle(order)
    return sorted(order, key=lambda o: -(min(o[0], side - o[0]) + min(o[1], side - o[1])))

def dot(a, b, dims=NN):
    return lax.dot_general(a, b, dims, preferred_element_type=F32)

def sigmoid(x):
    return 0.5 * jnp.tanh(0.5 * x) + 0.5

def norm_lanes(x):
    center = jnp.mean(x, axis=1, keepdims=True)
    shifted = x - center
    spread = jnp.mean(shifted * shifted, axis=1, keepdims=True)
    return shifted * lax.rsqrt(spread + EPSILON)

def iota(shape, dim):
    return lax.broadcasted_iota(jnp.int32, shape, dim)

def spread_rows(rows, picked, parity):
    return (iota((rows, picked), 0) == 2 * iota((rows, picked), 1) + parity).astype(F32).astype(BF)

def whole_wait(ref, sem):
    pltpu.make_async_copy(ref, ref, sem).wait()

def kernel(
    n,
    pair_hbm, mask_hbm, w_in_hbm, w_tg_hbm, w_to_hbm, w_qkv_hbm, w_ab_hbm, w_ag_hbm, w_ao_hbm,
    out_ref,
    pair_ref, mask_ref, w_in_ref, w_tg_ref, w_to_ref, w_qkv_ref, w_ab_ref, w_ag_ref, w_ao_ref,
    pair_send, pair_mid, pair_recv, edge_send, edge_mid, edge_recv, prod_send, prod_recv,
    tokens, middle, att_own, att_peer, bias_send, bias_recv, scores, o_send, o_recv, o_own, upd_send, upd_recv,
    load_sem, send_sem, recv_sem, edge_sem, pair_sem, bias_sem, ready_sem, late_sem, row_sem,
):
    loads = [
        pltpu.make_async_copy(hbm, ref, load_sem.at[i])
        for i, (hbm, ref) in enumerate(
            zip(
                (pair_hbm, mask_hbm, w_in_hbm, w_tg_hbm, w_to_hbm, w_qkv_hbm, w_ab_hbm, w_ag_hbm, w_ao_hbm),
                (pair_ref, mask_ref, w_in_ref, w_tg_ref, w_to_ref, w_qkv_ref, w_ab_ref, w_ag_ref, w_ao_ref),
            )
        )
    ]
    for load in loads:
        load.start()
    rows, res, cz = pair_ref.shape
    side = math.isqrt(n // 2)
    me = lax.axis_index("rows")
    core = lax.rem(me, 2)
    x = me // (2 * side)
    y = lax.rem(me // 2, side)
    partner = me + 1 - 2 * core
    lead = x + core * (y - x)
    far = sorted(range(1, side), key=lambda t: -min(t, side - t))
    near = sorted(range(1, side), key=lambda t: min(t, side - t))

    def chip(tx, ty):
        return lax.rem(x + tx, side) * side + lax.rem(y + ty, side)

    barrier = pltpu.get_barrier_semaphore()

    def greet(device):
        pl.semaphore_signal(barrier, inc=1, device_id={"rows": device}, device_id_type=MESH)

    first = me == 0
    in_row = (y == 0) & (x > 0)
    in_column = (x == 0) & (y > 0)
    feeds_first = in_row & (core == 0)
    ends_at_first = (in_column & (core == 0)) | (in_row & (core == 1))

    @pl.when(me > 0)
    def _():
        for t in far:

            @pl.when((y > 0) | (core == 1) | (lax.rem(x + t, side) > 0))
            def _():
                greet(2 * chip(t, 0))

            greet(2 * chip(0, t) + 1)
        greet(partner)

    def tell(sem, device):
        pl.semaphore_signal(sem, inc=1, device_id={"rows": device}, device_id_type=MESH)

    def push(source, target, sent, received, device):
        copy = pltpu.make_async_remote_copy(
            src_ref=source, dst_ref=target, send_sem=send_sem.at[sent], recv_sem=received,
            device_id={"rows": device}, device_id_type=MESH,
        )
        copy.start()

    def first_leg(send_ref, mid_ref, sent, sems):
        @pl.when(core == 0)
        def _():
            for t in far:
                target = lax.rem(x + t, side)

                @pl.when((y > 0) | (target > 0))
                def _():
                    push(
                        send_ref.at[target], mid_ref.at[x], sent, sems.at[(side - t) % side],
                        2 * (target * side + y),
                    )

        @pl.when(core == 1)
        def _():
            for t in far:
                push(
                    send_ref.at[:, lax.rem(y + t, side)], mid_ref.at[y], sent, sems.at[(side - t) % side],
                    2 * chip(0, t) + 1,
                )

    def around_first(send_ref, recv_ref, sent, received):
        for t in far + [0]:
            for c in range(2):
                if t or c:
                    push(send_ref.at[0, t, c], recv_ref.at[x, 0, 0], sent, received, 2 * t + c)

    def from_first(send_ref, recv_ref, sents, received):
        for tx, ty, tc in far_first(side):
            push(send_ref.at[tx, ty, tc], recv_ref.at[0, 0, 0], sents[tc], received, 2 * (tx * side + ty) + tc)
        pltpu.make_async_copy(send_ref.at[0, 0, 0], recv_ref.at[0, 0, 0], received).start()

    def own_leg(send_ref, mid_ref, sems):
        @pl.when(core == 0)
        def _():
            pltpu.make_async_copy(send_ref.at[x], mid_ref.at[x], sems.at[0]).start()

        @pl.when(core == 1)
        def _():
            pltpu.make_async_copy(send_ref.at[:, y], mid_ref.at[y], sems.at[0]).start()

    def second_leg(low, high, mid_ref, recv_ref, sent, sems, received, skip_first):
        span = pl.ds(low, high - low)
        for s in range(low, high):
            whole_wait(mid_ref.at[s], sems.at[lax.rem(s - lead + side, side)])
        for along in range(2):

            @pl.when(core == along)
            def _():
                target = recv_ref.at[x, span, 1] if along else recv_ref.at[span, y, 0]
                for t in far + [0]:
                    across = lax.rem((x if along else y) + t, side)
                    there = 2 * (chip(t, 0) if along else chip(0, t))
                    for c in (1 - along, along):
                        source = mid_ref.at[span, across, c]
                        if t and c == 0 and skip_first:

                            @pl.when(there > 0)
                            def _():
                                push(source, target, sent, received, there)
                        elif t or c != along:
                            push(source, target, sent, received, there + c)
                        else:
                            pltpu.make_async_copy(source, target, received).start()

    def second_leg_late(low, high, mid_ref, recv_ref, sent, received):
        span = pl.ds(low, high - low)
        for along in range(2):

            @pl.when(core == along)
            def _():
                target = recv_ref.at[x, span, 1] if along else recv_ref.at[span, y, 0]
                push(mid_ref.at[span, 0, 0], target, sent, received, 0)

    def exchange(source, target, k):
        for tx, ty, tc in far_first(side):
            d = 2 * chip(tx, ty) + core + tc - 2 * core * tc
            push(source(d), target, k, recv_sem.at[k], d)
        pltpu.make_async_copy(source(me), target, recv_sem.at[k]).start()

    def to_partner(source, target, k):
        push(source, target, k, recv_sem.at[k], partner)

    for load in loads[:3]:
        load.wait()

    key_mask = mask_ref[...].astype(F32)
    lane = iota((1, res), 1)
    row_mask = [
        jnp.sum(jnp.where(lane == me * rows + r, key_mask, 0.0), axis=1, keepdims=True) for r in range(rows)
    ]
    spreads = [spread_rows(2 * cz, cz, r) for r in range(2)]
    normed = jnp.concatenate(
        [norm_lanes(pair_ref[r].astype(F32)).astype(BF) for r in range(rows)], axis=1
    )

    def projected(g):
        w = w_in_ref[:, g * cz : (g + 1) * cz]
        spread_w = jnp.concatenate([dot(s, w, NT).astype(BF) for s in spreads], axis=1)
        return dot(spread_w, normed, NT)

    parity = iota((2 * cz, res), 0) % 2
    pair_mask = jnp.where(parity == 0, row_mask[0], row_mask[1]) * key_mask
    for a in range(2):
        edge = (sigmoid(projected(2 * a)) * projected(2 * a + 1) * pair_mask).astype(BF)
        edge_send[:, :, :, a] = edge.reshape(side, side, 2, 2, res)

    @pl.when(me > 0)
    def _():
        absent = feeds_first | ((x == 0) & (core == 1))
        pl.semaphore_wait(barrier, 2 * side - 1 - absent.astype(jnp.int32))

        @pl.when(me > 1)
        def _():
            tell(ready_sem, partner)

    edge_legs = (edge_mid, edge_recv, 0, edge_sem, recv_sem.at[0])
    pair_legs = (pair_mid, pair_recv, 1, pair_sem, recv_sem.at[1])
    spans = ((side // 2, side), (1, side // 2), (0, 1))

    @pl.when(first)
    def _():
        pl.semaphore_wait(barrier, 2 * side - 1)
        tell(ready_sem, 1)
        for t in far:
            for c in range(2):
                tell(late_sem, 2 * side * t + c)
            tell(late_sem, 2 * t)
        from_first(edge_send, edge_recv, (0, 8), recv_sem.at[0])

    @pl.when(me > 0)
    def _():
        first_leg(edge_send, edge_mid, 8, edge_sem)
        own_leg(edge_send, edge_mid, edge_sem)

    for r in range(rows):
        pair_send[:, :, :, r] = pair_ref[r].reshape(side, side, 2, 2, cz)
    for load in loads[3:]:
        load.wait()

    @pl.when(first)
    def _():
        from_first(pair_send, pair_recv, (1, 1), recv_sem.at[1])

    @pl.when(me > 0)
    def _():
        first_leg(pair_send, pair_mid, 9, pair_sem)
        own_leg(pair_send, pair_mid, pair_sem)
        pl.semaphore_wait(ready_sem, 1)

        @pl.when((core == 0) & (x > 0) & (y > 0))
        def _():
            tell(row_sem, 2 * side * x)

        @pl.when(feeds_first)
        def _():
            pl.semaphore_wait(row_sem, side - 1)
            greet(0)

        @pl.when(feeds_first)
        def _():
            for low, high in spans[:2]:
                second_leg(low, high, *edge_legs, True)
            around_first(edge_send, edge_recv, 8, recv_sem.at[0])
            around_first(pair_send, pair_recv, 9, recv_sem.at[1])
            pl.semaphore_wait(late_sem, 1)
            push(edge_send.at[0, 0, 0], edge_recv.at[x, 0, 0], 8, recv_sem.at[0], 0)
            push(pair_send.at[0, 0, 0], pair_recv.at[x, 0, 0], 9, recv_sem.at[1], 0)
            second_leg(1, side, *pair_legs, False)

        @pl.when(jnp.logical_not(feeds_first))
        def _():
            for low, high in ((side // 2, side), (0, side // 2)):
                second_leg(low, high, *edge_legs, True)

            @pl.when(ends_at_first)
            def _():
                pl.semaphore_wait(late_sem, 1)
                second_leg_late(0, side, edge_mid, edge_recv, 0, recv_sem.at[0])

            second_leg(0, side, *pair_legs, False)

    whole_wait(edge_recv, recv_sem.at[0])
    left = edge_recv[:, :, :, 0].reshape(res, res)
    right = edge_recv[:, :, :, 1].reshape(res, res)
    prod_send[...] = dot(right, left, NT).astype(BF).reshape(n, 2, res)
    exchange(lambda d: prod_send.at[d], prod_recv.at[me], 2)

    whole_wait(pair_recv, recv_sem.at[1])
    tokens[...] = pair_recv[...].reshape(2 * res, cz).astype(F32)
    columns = [tokens[pl.ds(jj, res, stride=2), :] for jj in range(2)]
    gates = [sigmoid(dot(norm_lanes(x).astype(BF), w_tg_ref[...])) for x in columns]
    w_to = w_to_ref[...]
    spread_out = jnp.concatenate([dot(s, w_to).astype(BF) for s in spreads], axis=1)
    e_row = iota((8, HEADS), 0)
    e_col = iota((8, HEADS), 1)
    w_bias = jnp.concatenate(
        [
            dot(((e_row // 2 == e_col) & (e_row % 2 == jj)).astype(F32).astype(BF), w_ab_ref[...]).astype(BF)
            for jj in range(2)
        ],
        axis=1,
    )

    whole_wait(prod_recv, recv_sem.at[2])
    product = prod_recv[...].reshape(2 * cz, res).astype(F32)
    sub = iota((8, res), 0) % 2

    def column_mean(x):
        total = jnp.sum(x.reshape(2 * cz // 8, 8, res), axis=0)
        even = jnp.sum(jnp.where(sub == 0, total, 0.0), axis=0, keepdims=True)
        odd = jnp.sum(jnp.where(sub == 0, 0.0, total), axis=0, keepdims=True)
        return jnp.where(sub == 0, even, odd) * (1.0 / cz)

    tall = product.reshape(2 * cz // 8, 8, res)
    tall = tall - column_mean(product)[None]
    spread = column_mean((tall * tall).reshape(2 * cz, res))
    tri = (tall * lax.rsqrt(spread + EPSILON)[None]).reshape(2 * cz, res).astype(BF)
    update = dot(tri, spread_out, TN)
    for jj in range(2):
        mid = (columns[jj] + gates[jj] * update[:, jj * cz : (jj + 1) * cz]).astype(BF).astype(F32)
        middle[jj] = mid
        att_own[jj] = norm_lanes(mid).astype(BF)
    to_partner(att_own, att_peer, 4)
    both = jnp.concatenate([att_own[0], att_own[1]], axis=1)
    bias_send[...] = dot(w_bias, both, NT).reshape(2, 4, res)
    for t in far:
        push(bias_send.at[0], bias_recv.at[me], 3, bias_sem.at[(side - t) % side], 2 * chip(t, 0))
        push(bias_send.at[1], bias_recv.at[me], 3, bias_sem.at[(side - t) % side], 2 * chip(0, t) + 1)
    push(bias_send.at[1 - core], bias_recv.at[me], 3, bias_sem.at[0], partner)
    pltpu.make_async_copy(bias_send.at[core], bias_recv.at[me], bias_sem.at[0]).start()

    def pass_on(u):
        s = lax.rem(lead + u, side)
        block = bias_recv.at[pl.ds(2 * ((s + core * (x - s)) * side + y + core * (s - y)), 2)]
        whole_wait(block, bias_sem.at[u])
        for t in far:
            push(block, block, 10, recv_sem.at[3], 2 * chip(core * t, (1 - core) * t) + core)

    penalty = (key_mask - 1.0) * MASK_PENALTY
    lane_head = iota((1, cz), 1) // HEAD_DIM
    head_mask = [lane_head == 2 * core + h for h in range(2)]
    values = []

    def score(rows_in):
        qkv = dot(rows_in, w_qkv_ref[...]).astype(BF)
        for h in range(2):
            key = jnp.where(head_mask[h], qkv[:, cz : 2 * cz], 0)
            scores[2 * len(values) + h] = dot(qkv[:, :cz], key, NT) * (HEAD_DIM ** -0.5) + penalty
        values.append(qkv[:, 2 * cz :])

    score(att_own[0])
    pass_on(0)
    score(att_own[1])
    whole_wait(att_peer, recv_sem.at[4])
    pass_on(near[0])
    pass_on(near[1])
    score(att_peer[0])
    pass_on(near[2])
    pass_on(near[3])
    score(att_peer[1])
    for u in near[4:]:
        pass_on(u)
    att_gates = [sigmoid(dot(att_own[jj], w_ag_ref[...])) for jj in range(2)]

    ones = [jnp.broadcast_to(jnp.where(m, 1.0, 0.0), (res, cz)).astype(BF) for m in head_mask]
    weighed = [[jnp.concatenate([jnp.where(head_mask[h], v, 0), ones[h]], axis=1) for h in range(2)] for v in values]
    whole_wait(bias_recv.at[pl.ds(0, n - 2 * side)], recv_sem.at[3])
    any_head = head_mask[0] | head_mask[1]
    biases = [bias_recv[:, 2 * h : 2 * h + 2].reshape(res, res) for h in range(2)]

    def attended(l):
        total = None
        for h in range(2):
            s = scores[2 * l + h] + biases[h]
            e = jnp.exp(s - jnp.max(s, axis=1, keepdims=True)).astype(BF)
            part = dot(e, weighed[l][h])
            total = part if total is None else total + part
        return (total[:, :cz] / jnp.where(any_head, total[:, cz:], 1.0)).astype(BF)

    for l in (2, 3):
        o_send[l - 2] = attended(l)
        to_partner(o_send.at[l - 2], o_recv.at[l - 2], 3 + l)
    for jj in range(2):
        o_own[jj] = attended(jj)
    for jj in range(2):
        middle[jj] = middle[jj] + dot((att_gates[jj] * o_own[jj].astype(F32)).astype(BF), w_ao_ref[...])
    for jj in range(2):
        whole_wait(o_recv.at[jj], recv_sem.at[5 + jj])
        gated = (att_gates[jj] * o_recv[jj].astype(F32)).astype(BF)
        tokens[pl.ds(jj, res, stride=2), :] = middle[jj] + dot(gated, w_ao_ref[...])
    upd_send[...] = tokens[...].astype(BF).reshape(n, rows, 2, cz)
    exchange(lambda d: upd_send.at[d], upd_recv.at[:, me], 7)
    whole_wait(upd_recv, recv_sem.at[7])
    out_ref[...] = upd_recv[...].reshape(rows, res, cz)

    others = pl.ds(0, n - 1)
    passed = pl.ds(0, n - side)

    half = pl.ds(0, res // 2)
    ahead = (side - 1) * (2 * side - 1)

    @pl.when(feeds_first)
    def _():
        whole_wait(bias_recv.at[pl.ds(0, ahead), :, half], send_sem.at[0])
        whole_wait(upd_send.at[pl.ds(0, ahead)], send_sem.at[1])

    @pl.when((me > 0) & jnp.logical_not(feeds_first))
    def _():
        whole_wait(bias_recv.at[passed, :, half], send_sem.at[0])
        whole_wait(upd_send.at[passed], send_sem.at[1])

    @pl.when(me > 0)
    def _():
        whole_wait(edge_mid.at[pl.ds(0, side - 1)], send_sem.at[8])
        whole_wait(pair_mid.at[pl.ds(0, side - 1)], send_sem.at[9])

    @pl.when(first)
    def _():
        whole_wait(prod_send.at[pl.ds(0, n - 2)], send_sem.at[0])
        whole_wait(prod_send, send_sem.at[8])
        whole_wait(upd_send.at[others], send_sem.at[1])

    whole_wait(prod_recv.at[others], send_sem.at[2])
    whole_wait(bias_recv.at[pl.ds(0, 2 * side - 1)], send_sem.at[3])
    whole_wait(att_peer, send_sem.at[4])
    whole_wait(o_recv.at[0], send_sem.at[5])
    whole_wait(o_recv.at[1], send_sem.at[6])
    whole_wait(upd_recv.at[:, others], send_sem.at[7])
    whole_wait(bias_recv.at[pl.ds(0, n - 2 * side)], send_sem.at[10])

def local(n, *args):
    args = [args[0], args[1].reshape(1, -1), *args[2:6], args[6].T, *args[7:]]
    rows, res, cz = args[0].shape
    side = math.isqrt(n // 2)
    pair_grid = (side, side, 2, rows, 2, cz)
    edge_grid = (side, side, 2, 2, 2, res)
    return pl.pallas_call(
        functools.partial(kernel, n),
        out_shape=pltpu.VMEM(args[0].shape, BF),
        in_specs=[pl.BlockSpec(memory_space=pl.ANY)] * len(args),
        out_specs=pl.BlockSpec(memory_space=pltpu.VMEM),
        scratch_shapes=[pltpu.VMEM(a.shape, a.dtype) for a in args]
        + [
            pltpu.VMEM(pair_grid, BF),
            pltpu.VMEM(pair_grid, BF),
            pltpu.VMEM(pair_grid, BF),
            pltpu.VMEM(edge_grid, BF),
            pltpu.VMEM(edge_grid, BF),
            pltpu.VMEM(edge_grid, BF),
            pltpu.VMEM((n, 2, res), BF),
            pltpu.VMEM((n, 2, res), BF),
            pltpu.VMEM((2 * res, cz), F32),
            pltpu.VMEM((2, res, cz), F32),
            pltpu.VMEM((2, res, cz), BF),
            pltpu.VMEM((2, res, cz), BF),
            pltpu.VMEM((2, 4, res), F32),
            pltpu.VMEM((n, 4, res), F32),
            pltpu.VMEM((8, res, res), F32),
            pltpu.VMEM((2, res, cz), BF),
            pltpu.VMEM((2, res, cz), BF),
            pltpu.VMEM((2, res, cz), BF),
            pltpu.VMEM((n, rows, 2, cz), BF),
            pltpu.VMEM((rows, n, 2, cz), BF),
            pltpu.SemaphoreType.DMA((len(args),)),
            pltpu.SemaphoreType.DMA((11,)),
            pltpu.SemaphoreType.DMA((8,)),
            pltpu.SemaphoreType.DMA((side,)),
            pltpu.SemaphoreType.DMA((side,)),
            pltpu.SemaphoreType.DMA((side,)),
            pltpu.SemaphoreType.REGULAR,
            pltpu.SemaphoreType.REGULAR,
            pltpu.SemaphoreType.REGULAR,
        ],
        compiler_params=pltpu.CompilerParams(collective_id=0, has_side_effects=True),
        name="pair_update",
    )(*args)

def solution(mesh):
    split = P(("parts", "rows"), None, None)
    placed = (split, P("parts"), P(), P(), P(), P(), P(), P(), P())
    return jax.shard_map(
        functools.partial(local, mesh.shape["rows"]), mesh=mesh, in_specs=placed, out_specs=split, check_vma=False
    )
```
